8 devices in a mesh: data: 2 (over z, y), cp: 4 (over x, core).
Axes of the slice: x: 2, y: 2, z: 1, core: 2. Of those that a mesh axis runs over, the one named last changes fastest.
Arguments:
- x_tokens: bfloat16 [32, 1024, 1536], P('data', 'cp'), parts along dimension 0
- positions: int32 [32, 1024], P('data', 'cp'), parts along dimension 0
- w_query: bfloat16 [1536, 1536], replicated
- w_key: bfloat16 [1536, 256], replicated
- w_value: bfloat16 [1536, 256], replicated
- w_out: bfloat16 [1536, 1536], replicated
Outputs:
- output: bfloat16 [32, 1024, 1536], P('data', 'cp'), parts along dimension 0
There are 2 independent parts. The reference program is written for one: setup_inputs(seed, part) draws one part's arguments, and reference() takes and returns one part's arrays. A program takes and returns all parts, laid end to end along the dimension named above; an argument that names none is the same for every part.
All inputs are finite; a program needn't handle non-finite values.
Results may differ from the reference program's by a relative error of at most 0.00437571.
Values are sent between devices in bfloat16 or wider.
A program may use at most 1 GiB of HBM per device.

```python
import jax
import jax.numpy as jnp
from jax import lax

BATCH_PART = 16
SEQ_LEN = 1024
CP_SIZE = 4
MODEL_DIM = 1536
Q_HEADS = 12
KV_HEADS = 2
HEAD_DIM = 128
ROPE_BASE = 500000
WALK_SEG = 16

GROUP_SIZE = Q_HEADS // KV_HEADS
HALF_LEN = SEQ_LEN // (2 * CP_SIZE)
BLOCK_LEN = min(HALF_LEN, 256)
BLOCK_COUNT = SEQ_LEN // BLOCK_LEN


def to_stored_order(seq_arr):
    tail_dims = seq_arr.shape[2:]
    blocks = seq_arr.reshape((BATCH_PART, 2 * CP_SIZE, HALF_LEN) + tail_dims)
    front_part = blocks[:, :CP_SIZE]
    back_part = jnp.flip(blocks[:, CP_SIZE:], axis=1)
    return jnp.stack([front_part, back_part], axis=2).reshape(seq_arr.shape)


def setup_inputs(seed: int = 0, part: int = 0) -> dict:
    root_key = jax.random.key(seed)
    k_query, k_key, k_value, k_out, k_part = jax.random.split(root_key, 5)
    part_key = jax.random.fold_in(k_part, part)
    k_noise, k_mean, k_walk, k_gap, k_start = jax.random.split(part_key, 5)
    seg_count = SEQ_LEN // WALK_SEG
    walk_steps = jax.random.normal(k_walk, (BATCH_PART, seg_count, MODEL_DIM), jnp.float32)
    walk_path = jnp.repeat(jnp.cumsum(walk_steps, axis=1) * (seg_count ** -0.5), WALK_SEG, axis=1)
    row_mean = jax.random.normal(k_mean, (BATCH_PART, 1, MODEL_DIM), jnp.float32)
    token_noise = jax.random.normal(k_noise, (BATCH_PART, SEQ_LEN, MODEL_DIM), jnp.float32)
    x_seq = 0.5 * token_noise + 0.5 * row_mean + walk_path
    pos_gaps = jax.random.randint(k_gap, (BATCH_PART, SEQ_LEN), 1, 4, dtype=jnp.int32)
    start_pos = jax.random.randint(k_start, (BATCH_PART, 1), 0, 1024, dtype=jnp.int32)
    pos_seq = start_pos + jnp.cumsum(pos_gaps, axis=1, dtype=jnp.int32)
    q_cols = Q_HEADS * HEAD_DIM
    kv_cols = KV_HEADS * HEAD_DIM
    w_query = (jax.random.normal(k_query, (MODEL_DIM, q_cols), jnp.float32) * MODEL_DIM ** -0.5).astype(jnp.bfloat16)
    w_key = (jax.random.normal(k_key, (MODEL_DIM, kv_cols), jnp.float32) * MODEL_DIM ** -0.5).astype(jnp.bfloat16)
    w_value = (jax.random.normal(k_value, (MODEL_DIM, kv_cols), jnp.float32) * MODEL_DIM ** -0.5).astype(jnp.bfloat16)
    w_out = (jax.random.normal(k_out, (q_cols, MODEL_DIM), jnp.float32) * (2.0 * q_cols ** -0.5)).astype(jnp.bfloat16)
    return {'x_tokens': to_stored_order(x_seq).astype(jnp.bfloat16), 'positions': to_stored_order(pos_seq), 'w_query': w_query, 'w_key': w_key, 'w_value': w_value, 'w_out': w_out}


def apply_rope(head_vecs, positions):
    half_dim = HEAD_DIM // 2
    inv_freq = 1.0 / (ROPE_BASE ** (jnp.arange(0, HEAD_DIM, 2, dtype=jnp.float32) / HEAD_DIM))
    angles = positions.astype(jnp.float32)[:, :, None] * inv_freq
    tab_shape = angles.shape[:2] + (1,) * (head_vecs.ndim - 3) + (half_dim,)
    cosine = jnp.cos(angles).reshape(tab_shape)
    sine_tab = jnp.sin(angles).reshape(tab_shape)
    lower_half = head_vecs[..., :half_dim].astype(jnp.float32)
    upper_half = head_vecs[..., half_dim:].astype(jnp.float32)
    rotated = jnp.concatenate([lower_half * cosine - upper_half * sine_tab, upper_half * cosine + lower_half * sine_tab], axis=-1)
    return rotated.astype(jnp.bfloat16)


def reference(x_tokens, positions, w_query, w_key, w_value, w_out):
    score_scale = HEAD_DIM ** -0.5
    mask_fill = -1e30
    flat_x = x_tokens.reshape(BATCH_PART * SEQ_LEN, MODEL_DIM)
    q_proj = jnp.dot(flat_x, w_query, preferred_element_type=jnp.float32).astype(jnp.bfloat16)
    k_proj = jnp.dot(flat_x, w_key, preferred_element_type=jnp.float32).astype(jnp.bfloat16)
    v_proj = jnp.dot(flat_x, w_value, preferred_element_type=jnp.float32).astype(jnp.bfloat16)
    q_rot = apply_rope(q_proj.reshape(BATCH_PART, SEQ_LEN, KV_HEADS, GROUP_SIZE, HEAD_DIM), positions)
    k_rot = apply_rope(k_proj.reshape(BATCH_PART, SEQ_LEN, KV_HEADS, HEAD_DIM), positions)
    v_rows = v_proj.reshape(BATCH_PART, SEQ_LEN, KV_HEADS, HEAD_DIM)
    q_blocks = jnp.moveaxis(q_rot.reshape(BATCH_PART, BLOCK_COUNT, BLOCK_LEN, KV_HEADS, GROUP_SIZE, HEAD_DIM), 1, 0)
    k_blocks = jnp.moveaxis(k_rot.reshape(BATCH_PART, BLOCK_COUNT, BLOCK_LEN, KV_HEADS, HEAD_DIM), 1, 0)
    v_blocks = jnp.moveaxis(v_rows.reshape(BATCH_PART, BLOCK_COUNT, BLOCK_LEN, KV_HEADS, HEAD_DIM), 1, 0)
    pos_blocks = jnp.moveaxis(positions.reshape(BATCH_PART, BLOCK_COUNT, BLOCK_LEN), 1, 0)

    def query_block(block_in):
        q_blk, q_pos = block_in
        q_wide = q_blk.astype(jnp.float32)

        def key_step(carry_state, key_in):
            m_run, l_run, acc_run = carry_state
            k_blk, v_blk, k_pos = key_in
            scores = jnp.einsum('bqhgd,bkhd->bhgqk', q_wide, k_blk.astype(jnp.float32)) * score_scale
            allowed = (k_pos[:, None, :] <= q_pos[:, :, None])[:, None, None]
            scores = jnp.where(allowed, scores, mask_fill)
            m_new = jnp.maximum(m_run, jnp.max(scores, axis=-1))
            exp_w = jnp.where(allowed, jnp.exp(scores - m_new[..., None]), 0.0)
            rescale = jnp.exp(m_run - m_new)
            l_new = rescale * l_run + jnp.sum(exp_w, axis=-1)
            pv_part = jnp.einsum('bhgqk,bkhd->bhgqd', exp_w.astype(jnp.bfloat16).astype(jnp.float32), v_blk.astype(jnp.float32))
            return (m_new, l_new, rescale[..., None] * acc_run + pv_part), None

        state_shape = (BATCH_PART, KV_HEADS, GROUP_SIZE, BLOCK_LEN)
        init_state = (jnp.full(state_shape, mask_fill, jnp.float32), jnp.zeros(state_shape, jnp.float32), jnp.zeros(state_shape + (HEAD_DIM,), jnp.float32))
        final_state, _ = lax.scan(key_step, init_state, (k_blocks, v_blocks, pos_blocks))
        attn_out = (final_state[2] / final_state[1][..., None]).astype(jnp.bfloat16)
        return attn_out.transpose(0, 3, 1, 2, 4)

    attn_all = lax.map(query_block, (q_blocks, pos_blocks))
    attn_rows = jnp.moveaxis(attn_all, 0, 1).reshape(BATCH_PART * SEQ_LEN, Q_HEADS * HEAD_DIM)
    out_proj = jnp.dot(attn_rows, w_out, preferred_element_type=jnp.float32).reshape(BATCH_PART, SEQ_LEN, MODEL_DIM)
    return (x_tokens.astype(jnp.float32) + out_proj).astype(jnp.bfloat16)
```

```python
import functools
import math

import jax
import jax.numpy as jnp
from jax import lax
from jax.experimental import pallas as pl
from jax.experimental.pallas import tpu as pltpu
from jax.sharding import PartitionSpec as P

HEAD_DIM = 128
HALF_DIM = HEAD_DIM // 2
ROPE_BASE = 500000
MASK_FILL = -1e30
EXP_SCALE = math.log2(math.e) * HEAD_DIM ** -0.5
CP_SIZE = 4
BLK = 128
MESH = pl.DeviceIdType.MESH


def nt_dot(lhs, rhs):
    return lax.dot_general(lhs, rhs, (((1,), (1,)), ((), ())), preferred_element_type=jnp.float32)


def rope_head(head, cos_tab, sin_tab):
    wide = head.astype(jnp.float32)
    return (wide * cos_tab + pltpu.roll(wide, HALF_DIM, 1) * sin_tab).astype(jnp.bfloat16)


def kernel(x_hbm, pos_ref, freq_ref, wq_hbm, wk_hbm, wv_hbm, wo_hbm, y_hbm,
           xb, wq, wk, wv, wo, kv, qb, ob, cos_b, sin_b,
           xsem, wsem, ysem, ici_s, ici_r, sib_s, sib_r, fwd_s, fwd_r):
    rows, toks, width = xb.shape
    kv_cols = wk.shape[1]
    kv_heads = kv_cols // HEAD_DIM
    q_heads = wq.shape[1] // HEAD_DIM
    group = q_heads // kv_heads
    me = lax.axis_index("cp")
    chip = me // 2
    core = lax.rem(me, 2)
    sib = chip * 2 + (1 - core)
    par = (1 - chip) * 2 + core
    dia = (1 - chip) * 2 + (1 - core)
    last = 2 * CP_SIZE - 1

    w_copies = [pltpu.make_async_copy(src, dst, wsem.at[i]) for i, (src, dst) in enumerate(((wk_hbm, wk), (wv_hbm, wv), (wq_hbm, wq), (wo_hbm, wo)))]

    def x_copy(b):
        return pltpu.make_async_copy(x_hbm.at[b], xb.at[b], xsem.at[b])

    def y_copy(b):
        return pltpu.make_async_copy(xb.at[b], y_hbm.at[b], ysem.at[b])

    w_copies[0].start()
    x_copy(0).start()
    w_copies[1].start()
    for b in range(1, 3):
        x_copy(b).start()
    w_copies[2].start()
    for b in range(3, rows):
        x_copy(b).start()
    w_copies[3].start()

    barrier = pltpu.get_barrier_semaphore()
    for other in (sib, par):
        pl.semaphore_signal(barrier, inc=1, device_id={"cp": other}, device_id_type=MESH)
    pl.semaphore_wait(barrier, 2)

    def block(b, idx):
        return kv.at[b, pl.ds(pl.multiple_of(idx * BLK, BLK), BLK), :]

    def remote(b, idx, half, send, recv, dev):
        return pltpu.make_async_remote_copy(src_ref=block(b, idx), dst_ref=block(b, idx), send_sem=send.at[half, b], recv_sem=recv.at[half, b], device_id={"cp": dev}, device_id_type=MESH)

    def send_row(b):
        remote(b, me, 0, ici_s, ici_r, par).start()

        @pl.when(chip == 1)
        def _():
            remote(b, last - me, 1, ici_s, ici_r, par).start()

        remote(b, me, 0, sib_s, sib_r, sib).start()

        @pl.when(core == 1)
        def _():
            remote(b, last - me, 1, sib_s, sib_r, sib).start()

    def make_kv(b):
        angles = freq_ref[...] * pos_ref[pl.ds(b, 1), :].astype(jnp.float32)
        cosine, sine = jnp.cos(angles), jnp.sin(angles)
        cos_tab = jnp.concatenate([cosine, cosine], axis=0).T
        sin_tab = jnp.concatenate([-sine, sine], axis=0).T
        cos_b[b] = cos_tab
        sin_b[b] = sin_tab
        x_row = xb[b]
        k_row = jnp.dot(x_row, wk[...], preferred_element_type=jnp.float32).astype(jnp.bfloat16)
        v_row = jnp.dot(x_row, wv[...], preferred_element_type=jnp.float32).astype(jnp.bfloat16)
        for half, idx in ((0, me), (1, last - me)):
            lo = half * BLK
            dst = pl.ds(pl.multiple_of(idx * BLK, BLK), BLK)
            for h in range(kv_heads):
                cols = slice(h * HEAD_DIM, (h + 1) * HEAD_DIM)
                kv[b, dst, cols] = rope_head(k_row[lo:lo + BLK, cols], cos_tab[lo:lo + BLK], sin_tab[lo:lo + BLK])
            kv[b, dst, kv_cols:] = v_row[lo:lo + BLK]

    def make_q(b, slot):
        x_row = xb[b]
        cos_tab, sin_tab = cos_b[b], sin_b[b]
        for n in range(0, q_heads, 2):
            pair = jnp.dot(x_row, wq[:, n * HEAD_DIM:(n + 2) * HEAD_DIM], preferred_element_type=jnp.float32).astype(jnp.bfloat16)
            for i in range(2):
                qb[slot, n + i] = rope_head(pair[:, i * HEAD_DIM:(i + 1) * HEAD_DIM], cos_tab, sin_tab)

    def attend(b, slot, dev):
        tri = lax.broadcasted_iota(jnp.int32, (2 * BLK, BLK), 1) <= lax.rem(lax.broadcasted_iota(jnp.int32, (2 * BLK, BLK), 0), BLK)
        for g in range(kv_heads):
            for half, n_blk in ((1, last - dev + 1), (0, dev + 1)):
                n_key = n_blk * BLK
                toks_at = slice(half * BLK, (half + 1) * BLK)
                keys = kv[b, 0:n_key, g * HEAD_DIM:(g + 1) * HEAD_DIM]
                vals = kv[b, 0:n_key, kv_cols + g * HEAD_DIM:kv_cols + (g + 1) * HEAD_DIM]
                for h in range(g * group, (g + 1) * group, 2):
                    q_pair = qb[slot, h:h + 2, toks_at, :].reshape(2 * BLK, HEAD_DIM)
                    scores = nt_dot(q_pair, keys)
                    diag = jnp.where(tri, scores[:, n_key - BLK:], MASK_FILL)
                    scores = diag if n_blk == 1 else jnp.concatenate([scores[:, :n_key - BLK], diag], axis=1)
                    top = jnp.max(scores, axis=1, keepdims=True)
                    exp_w = jnp.exp2((scores - top) * EXP_SCALE)
                    inv = 1.0 / jnp.sum(exp_w, axis=1, keepdims=True)
                    out = (jnp.dot(exp_w.astype(jnp.bfloat16), vals, preferred_element_type=jnp.float32) * inv).astype(jnp.bfloat16)
                    for i in range(2):
                        ob[toks_at, (h + i) * HEAD_DIM:(h + i + 1) * HEAD_DIM] = out[i * BLK:(i + 1) * BLK]

    def project_out(b):
        o_row = ob[...]
        for n in range(0, width, 2 * HEAD_DIM):
            cols = slice(n, n + 2 * HEAD_DIM)
            y_part = jnp.dot(o_row, wo[:, cols], preferred_element_type=jnp.float32)
            xb[b, :, cols] = (xb[b, :, cols].astype(jnp.float32) + y_part).astype(jnp.bfloat16)
        y_copy(b).start()

    w_copies[0].wait()
    w_copies[1].wait()

    def kv_step(b, _):
        x_copy(b).wait()
        make_kv(b)

        @pl.when(b > 0)
        def _():
            send_row(b - 1)

        return _

    lax.fori_loop(0, rows, kv_step, None)
    send_row(rows - 1)
    w_copies[2].wait()
    make_q(0, 0)
    w_copies[3].wait()

    def row_step(b, _):
        slot = lax.rem(b, 2)
        remote(b, par, 0, ici_s, ici_r, par).wait_recv()
        remote(b, par, 0, fwd_s, fwd_r, sib).start()

        @pl.when(chip == 0)
        def _():
            remote(b, last - par, 1, ici_s, ici_r, par).wait_recv()
            remote(b, last - par, 1, fwd_s, fwd_r, sib).start()

        @pl.when(b < rows - 1)
        def _():
            make_q(b + 1, 1 - slot)

        remote(b, sib, 0, sib_s, sib_r, sib).wait_recv()

        @pl.when(core == 0)
        def _():
            remote(b, last - sib, 1, sib_s, sib_r, sib).wait_recv()

        remote(b, dia, 0, fwd_s, fwd_r, sib).wait_recv()

        @pl.when(chip == 0)
        def _():
            remote(b, last - dia, 1, fwd_s, fwd_r, sib).wait_recv()

        for dev in range(CP_SIZE):
            @pl.when(me == dev)
            def _():
                attend(b, slot, dev)

        project_out(b)
        return _

    lax.fori_loop(0, rows, row_step, None)

    def drain(b, _):
        y_copy(b).wait()
        remote(b, me, 0, ici_s, ici_r, par).wait_send()
        remote(b, me, 0, sib_s, sib_r, sib).wait_send()
        remote(b, par, 0, fwd_s, fwd_r, sib).wait_send()

        @pl.when(chip == 1)
        def _():
            remote(b, last - me, 1, ici_s, ici_r, par).wait_send()

        @pl.when(core == 1)
        def _():
            remote(b, last - me, 1, sib_s, sib_r, sib).wait_send()

        @pl.when(chip == 0)
        def _():
            remote(b, last - par, 1, fwd_s, fwd_r, sib).wait_send()

        return _

    lax.fori_loop(0, rows, drain, None)


def solution(mesh):
    row_spec = P('data', 'cp', None)
    pos_spec = P('data', 'cp')
    rep_spec = P(None, None)

    def local_block(x_loc, pos_loc, w_query, w_key, w_value, w_out):
        rows, toks, width = x_loc.shape
        q_cols, kv_cols = w_query.shape[1], w_key.shape[1]
        inv_freq = 1.0 / (ROPE_BASE ** (jnp.arange(0, HEAD_DIM, 2, dtype=jnp.float32) / HEAD_DIM))
        freq = jnp.broadcast_to(inv_freq[:, None], (HALF_DIM, toks))
        any_spec = pl.BlockSpec(memory_space=pl.ANY)
        vmem_spec = pl.BlockSpec(memory_space=pltpu.VMEM)
        bf16, f32 = jnp.bfloat16, jnp.float32
        pair_sem = pltpu.SemaphoreType.DMA((2, rows))
        row_sem = pltpu.SemaphoreType.DMA((rows,))
        return pl.pallas_call(
            kernel,
            out_shape=jax.ShapeDtypeStruct(x_loc.shape, bf16),
            in_specs=[any_spec, vmem_spec, vmem_spec] + [any_spec] * 4,
            out_specs=any_spec,
            scratch_shapes=[
                pltpu.VMEM((rows, toks, width), bf16),
                pltpu.VMEM((width, q_cols), bf16),
                pltpu.VMEM((width, kv_cols), bf16),
                pltpu.VMEM((width, kv_cols), bf16),
                pltpu.VMEM((q_cols, width), bf16),
                pltpu.VMEM((rows, CP_SIZE * toks, 2 * kv_cols), bf16),
                pltpu.VMEM((2, q_cols // HEAD_DIM, toks, HEAD_DIM), bf16),
                pltpu.VMEM((toks, q_cols), bf16),
                pltpu.VMEM((rows, toks, HEAD_DIM), f32),
                pltpu.VMEM((rows, toks, HEAD_DIM), f32),
                row_sem, pltpu.SemaphoreType.DMA((4,)), row_sem,
                pair_sem, pair_sem, pair_sem, pair_sem, pair_sem, pair_sem,
            ],
            compiler_params=pltpu.CompilerParams(collective_id=0, has_side_effects=True, vmem_limit_bytes=62 * 1024 * 1024),
        )(x_loc, pos_loc, freq, w_query, w_key, w_value, w_out)

    return jax.shard_map(local_block, mesh=mesh, in_specs=(row_spec, pos_spec, rep_spec, rep_spec, rep_spec, rep_spec), out_specs=row_spec, check_vma=False)
```

```python
import functools
import math

import jax
import jax.numpy as jnp
import numpy as np
from jax import lax
from jax.experimental import pallas as pl
from jax.experimental.pallas import tpu as pltpu
from jax.sharding import PartitionSpec as P

HEAD_DIM = 128
HALF_DIM = HEAD_DIM // 2
ROPE_BASE = 500000
MASK_FILL = -1e30
EXP_SCALE = math.log2(math.e) * HEAD_DIM ** -0.5
CP_SIZE = 4
BLK = 128
MESH = pl.DeviceIdType.MESH
TURN = 2.0 ** 32
SIN_COEF = [(-1) ** k * (2 * math.pi) ** (2 * k + 1) / math.factorial(2 * k + 1) for k in range(7)]


def turn_tables(toks):
    turns = ROPE_BASE ** (-np.arange(0, HEAD_DIM, 2, dtype=np.float64) / HEAD_DIM) / (2 * math.pi)
    high = np.floor(turns * TURN)
    low = turns - high / TURN
    sub = 8
    lane_row = lax.broadcasted_iota(jnp.int32, (sub, toks), 0)
    parts = ([], [])
    for a in range(0, HALF_DIM, sub):
        for part, values, kind, num in zip(parts, (high, low), (jnp.int32, jnp.float32), (int, float)):
            tile = jnp.full((sub, toks), num(values[a]), kind)
            for c in range(1, sub):
                tile = jnp.where(lane_row == c, jnp.full((sub, toks), num(values[a + c]), kind), tile)
            part.append(tile)
    return [jnp.concatenate(part, axis=0) for part in parts]


def sin_turns(part):
    square = part * part
    total = jnp.full_like(part, SIN_COEF[-1])
    for coef in SIN_COEF[-2::-1]:
        total = total * square + coef
    return total * part


def nt_dot(lhs, rhs):
    return lax.dot_general(lhs, rhs, (((1,), (1,)), ((), ())), preferred_element_type=jnp.float32)


def rope_head(head, cos_tab, sin_tab):
    wide = head.astype(jnp.float32)
    return (wide * cos_tab + pltpu.roll(wide, HALF_DIM, 1) * sin_tab).astype(jnp.bfloat16)


def kernel(x_hbm, pos_ref, wq_hbm, wk_hbm, wv_hbm, wo_hbm, xb,
           wq, wk, wv, wo, kv, qb, ob, sb, high_b, low_b, cos_b, sin_b,
           xsem, wsem, ici_s, ici_r, sib_s, sib_r, fwd_s, fwd_r):
    rows, toks, width = xb.shape
    kv_cols = wk.shape[1]
    kv_heads = kv_cols // HEAD_DIM
    q_heads = wq.shape[1] // HEAD_DIM
    group = q_heads // kv_heads
    me = lax.axis_index("cp")
    chip = me // 2
    core = lax.rem(me, 2)
    sib = chip * 2 + (1 - core)
    par = (1 - chip) * 2 + core
    dia = (1 - chip) * 2 + (1 - core)
    last = 2 * CP_SIZE - 1

    w_copies = [pltpu.make_async_copy(src, dst, wsem.at[i]) for i, (src, dst) in enumerate(((wk_hbm, wk), (wv_hbm, wv), (wq_hbm, wq), (wo_hbm, wo)))]

    def x_copy(b):
        return pltpu.make_async_copy(x_hbm.at[b], xb.at[b], xsem.at[b])

    def w_piece(src, dst, i, at):
        depth = src.shape[0] // (rows // 2)
        part = pl.ds(pl.multiple_of(at * depth, depth), depth)
        return pltpu.make_async_copy(src.at[part], dst.at[part], wsem.at[i])

    w_copies[0].start()
    x_copy(0).start()
    w_copies[1].start()
    x_copy(1).start()
    high_b[...], low_b[...] = turn_tables(toks)
    barrier = pltpu.get_barrier_semaphore()
    for other in (sib, par):
        pl.semaphore_signal(barrier, inc=1, device_id={"cp": other}, device_id_type=MESH)
    pl.semaphore_wait(barrier, 2)

    def block(b, idx):
        return kv.at[b, idx]

    def remote(b, idx, half, send, recv, dev):
        return pltpu.make_async_remote_copy(src_ref=block(b, idx), dst_ref=block(b, idx), send_sem=send.at[half, b], recv_sem=recv.at[half, b], device_id={"cp": dev}, device_id_type=MESH)

    def send_row(b):
        remote(b, me, 0, ici_s, ici_r, par).start()

        @pl.when(chip == 1)
        def _():
            remote(b, last - me, 1, ici_s, ici_r, par).start()

        remote(b, me, 0, sib_s, sib_r, sib).start()

        @pl.when(core == 1)
        def _():
            remote(b, last - me, 1, sib_s, sib_r, sib).start()

    def make_kv(b):
        pos = pos_ref[pl.ds(b, 1), :]
        turns = (pos * high_b[...]).astype(jnp.float32) * (1.0 / TURN) + pos.astype(jnp.float32) * low_b[...]
        turns = turns - jnp.round(turns)
        size = jnp.abs(turns)
        cosine = sin_turns(0.25 - size)
        sine = sin_turns(jnp.minimum(size, 0.5 - size))
        sine = jnp.where(turns < 0, -sine, sine)
        cos_tab = jnp.concatenate([cosine, cosine], axis=0).T
        sin_tab = jnp.concatenate([-sine, sine], axis=0).T
        cos_b[b] = cos_tab
        sin_b[b] = sin_tab
        x_row = xb[b]
        k_row = jnp.dot(x_row, wk[...], preferred_element_type=jnp.float32).astype(jnp.bfloat16)
        v_row = jnp.dot(x_row, wv[...], preferred_element_type=jnp.float32)
        for half, idx in ((0, me), (1, last - me)):
            lo = half * BLK
            for h in range(kv_heads):
                cols = slice(h * HEAD_DIM, (h + 1) * HEAD_DIM)
                kv[b, idx, cols, :] = rope_head(k_row[lo:lo + BLK, cols], cos_tab[lo:lo + BLK], sin_tab[lo:lo + BLK])
                kv[b, idx, kv_cols + h * HEAD_DIM:kv_cols + (h + 1) * HEAD_DIM, :] = v_row[lo:lo + BLK, cols].T.astype(jnp.bfloat16)

    def make_q(b, slot):
        x_row = xb[b]
        cos_tab, sin_tab = cos_b[b], sin_b[b]
        for n in range(0, q_heads, 2):
            pair = jnp.dot(x_row, wq[:, n * HEAD_DIM:(n + 2) * HEAD_DIM], preferred_element_type=jnp.float32).astype(jnp.bfloat16)
            for i in range(2):
                qb[slot, n + i] = rope_head(pair[:, i * HEAD_DIM:(i + 1) * HEAD_DIM], cos_tab, sin_tab)

    def attend(b, slot, dev, fill):
        wide = (BLK, 2 * BLK)
        tri = lax.broadcasted_iota(jnp.int32, wide, 0) <= lax.rem(lax.broadcasted_iota(jnp.int32, wide, 1), BLK)
        units = [(half, g, h) for half in (1, 0) for g in range(kv_heads) for h in range(g * group, (g + 1) * group, 2)]

        def spans(half):
            n_blk = last - dev + 1 if half else dev + 1
            return n_blk, n_blk * BLK, slice(half * BLK, (half + 1) * BLK)

        def score(k):
            half, g, h = units[k]
            n_blk, n_key, toks_at = spans(half)
            keys = kv[b, 0:n_blk, g * HEAD_DIM:(g + 1) * HEAD_DIM, :].reshape(n_key, HEAD_DIM)
            scores = nt_dot(keys, qb[slot, h:h + 2, toks_at, :].reshape(2 * BLK, HEAD_DIM))
            diag = jnp.where(tri, scores[n_key - BLK:], MASK_FILL)
            sb[k % 2, n_key - BLK:n_key, :] = diag
            top = jnp.max(diag, axis=0, keepdims=True)
            if n_blk > 1:
                sb[k % 2, 0:n_key - BLK, :] = scores[:n_key - BLK]
                top = jnp.maximum(top, jnp.max(scores[:n_key - BLK], axis=0, keepdims=True))
            return top

        def weigh(k, top):
            half, g, h = units[k]
            n_blk, n_key, toks_at = spans(half)
            exp_w = jnp.exp2((sb[k % 2, 0:n_key, :] - top) * EXP_SCALE)
            inv = 1.0 / jnp.sum(exp_w, axis=0, keepdims=True)
            rows_at = slice(kv_cols + g * HEAD_DIM, kv_cols + (g + 1) * HEAD_DIM)
            vals = jnp.concatenate([kv[b, i, rows_at, :] for i in range(n_blk)], axis=1)
            out = (jnp.dot(vals, exp_w.astype(jnp.bfloat16), preferred_element_type=jnp.float32) * inv).T.astype(jnp.bfloat16)
            for i in range(2):
                ob[slot, toks_at, (h + i) * HEAD_DIM:(h + i + 1) * HEAD_DIM] = out[i * BLK:(i + 1) * BLK]

        top = score(0)
        for k in range(len(units)):
            ahead = score(k + 1) if k + 1 < len(units) else None
            weigh(k, top)
            top = ahead
            fill(k, len(units))

    def out_tile(b, slot, n, keep):
        cols = slice(n * 2 * HEAD_DIM, (n + 1) * 2 * HEAD_DIM)
        y_part = jnp.dot(ob[slot], wo[:, cols], preferred_element_type=jnp.float32)
        if keep is not None:
            y_part = jnp.where(keep, y_part, 0.0)
        xb[b, :, cols] = (xb[b, :, cols].astype(jnp.float32) + y_part).astype(jnp.bfloat16)

    out_tiles = width // (2 * HEAD_DIM)

    w_copies[0].wait()
    w_copies[1].wait()

    def kv_step(b, _):
        @pl.when(b < rows - 2)
        def _():
            x_copy(b + 2).start()

        @pl.when(b < rows // 2)
        def _():
            w_piece(wq_hbm, wq, 2, b).start()

        @pl.when(b >= rows // 2)
        def _():
            w_piece(wo_hbm, wo, 3, b - rows // 2).start()

        x_copy(b).wait()
        make_kv(b)

        @pl.when(b > 0)
        def _():
            send_row(b - 1)

        return _

    lax.fori_loop(0, rows, kv_step, None)
    send_row(rows - 1)
    w_copies[2].wait()
    make_q(0, 0)
    w_copies[3].wait()

    def row_step(b, _):
        slot = lax.rem(b, 2)
        remote(b, par, 0, ici_s, ici_r, par).wait_recv()
        remote(b, par, 0, fwd_s, fwd_r, sib).start()

        @pl.when(chip == 0)
        def _():
            remote(b, last - par, 1, ici_s, ici_r, par).wait_recv()
            remote(b, last - par, 1, fwd_s, fwd_r, sib).start()

        @pl.when(b < rows - 1)
        def _():
            make_q(b + 1, 1 - slot)

        remote(b, sib, 0, sib_s, sib_r, sib).wait_recv()

        @pl.when(core == 0)
        def _():
            remote(b, last - sib, 1, sib_s, sib_r, sib).wait_recv()

        remote(b, dia, 0, fwd_s, fwd_r, sib).wait_recv()

        @pl.when(chip == 0)
        def _():
            remote(b, last - dia, 1, fwd_s, fwd_r, sib).wait_recv()

        def fill(k, count):
            if (k + 1) * out_tiles // count > k * out_tiles // count:
                out_tile(jnp.maximum(b - 1, 0), 1 - slot, k * out_tiles // count, b > 0)

        for dev in range(CP_SIZE):
            @pl.when(me == dev)
            def _():
                attend(b, slot, dev, fill)

        return _

    lax.fori_loop(0, rows, row_step, None)
    for n in range(out_tiles):
        out_tile(rows - 1, (rows - 1) % 2, n, None)

    def drain(b, _):
        remote(b, me, 0, ici_s, ici_r, par).wait_send()
        remote(b, me, 0, sib_s, sib_r, sib).wait_send()
        remote(b, par, 0, fwd_s, fwd_r, sib).wait_send()

        @pl.when(chip == 1)
        def _():
            remote(b, last - me, 1, ici_s, ici_r, par).wait_send()

        @pl.when(core == 1)
        def _():
            remote(b, last - me, 1, sib_s, sib_r, sib).wait_send()

        @pl.when(chip == 0)
        def _():
            remote(b, last - par, 1, fwd_s, fwd_r, sib).wait_send()

        return _

    lax.fori_loop(0, rows, drain, None)


def put_kernel(y_vmem, y_hbm, sem):
    rows = y_vmem.shape[0]
    copies = [pltpu.make_async_copy(y_vmem.at[b], y_hbm.at[b], sem.at[b]) for b in range(rows)]
    for copy in copies:
        copy.start()
    for copy in copies:
        copy.wait()


def put_out(y_vmem):
    return pl.pallas_call(
        put_kernel,
        out_shape=jax.ShapeDtypeStruct(y_vmem.shape, y_vmem.dtype),
        in_specs=[pl.BlockSpec(memory_space=pltpu.VMEM)],
        out_specs=pl.BlockSpec(memory_space=pl.ANY),
        scratch_shapes=[pltpu.SemaphoreType.DMA((y_vmem.shape[0],))],
        compiler_params=pltpu.CompilerParams(vmem_limit_bytes=14 * 1024 * 1024),
    )(y_vmem)


def solution(mesh):
    row_spec = P('data', 'cp', None)
    pos_spec = P('data', 'cp')
    rep_spec = P(None, None)

    def local_block(x_loc, pos_loc, w_query, w_key, w_value, w_out):
        rows, toks, width = x_loc.shape
        q_cols, kv_cols = w_query.shape[1], w_key.shape[1]
        any_spec = pl.BlockSpec(memory_space=pl.ANY)
        vmem_spec = pl.BlockSpec(memory_space=pltpu.VMEM)
        bf16, f32 = jnp.bfloat16, jnp.float32
        pair_sem = pltpu.SemaphoreType.DMA((2, rows))
        row_sem = pltpu.SemaphoreType.DMA((rows,))
        y_vmem = pl.pallas_call(
            kernel,
            out_shape=pltpu.VMEM(x_loc.shape, bf16),
            in_specs=[any_spec, vmem_spec] + [any_spec] * 4,
            out_specs=vmem_spec,
            scratch_shapes=[
                pltpu.VMEM((width, q_cols), bf16),
                pltpu.VMEM((width, kv_cols), bf16),
                pltpu.VMEM((width, kv_cols), bf16),
                pltpu.VMEM((q_cols, width), bf16),
                pltpu.VMEM((rows, 2 * CP_SIZE, 2 * kv_cols, BLK), bf16),
                pltpu.VMEM((2, q_cols // HEAD_DIM, toks, HEAD_DIM), bf16),
                pltpu.VMEM((2, toks, q_cols), bf16),
                pltpu.VMEM((2, CP_SIZE * toks, 2 * BLK), f32),
                pltpu.VMEM((HALF_DIM, toks), jnp.int32),
                pltpu.VMEM((HALF_DIM, toks), f32),
                pltpu.VMEM((rows, toks, HEAD_DIM), f32),
                pltpu.VMEM((rows, toks, HEAD_DIM), f32),
                row_sem, pltpu.SemaphoreType.DMA((4,)),
                pair_sem, pair_sem, pair_sem, pair_sem, pair_sem, pair_sem,
            ],
            compiler_params=pltpu.CompilerParams(collective_id=0, has_side_effects=True, vmem_limit_bytes=48 * 1024 * 1024),
        )(x_loc, pos_loc, w_query, w_key, w_value, w_out)
        return put_out(y_vmem)

    return jax.shard_map(local_block, mesh=mesh, in_specs=(row_spec, pos_spec, rep_spec, rep_spec, rep_spec, rep_spec), out_specs=row_spec, check_vma=False)
```

```python
import math

import jax
import jax.numpy as jnp
import numpy as np
from jax import lax
from jax.experimental import pallas as pl
from jax.experimental.pallas import tpu as pltpu
from jax.sharding import PartitionSpec as P

HEAD_DIM = 128
HALF_DIM = HEAD_DIM // 2
ROPE_BASE = 500000
MASK_FILL = -1e30
EXP_SCALE = math.log2(math.e) * HEAD_DIM ** -0.5
CP_SIZE = 4
LAST = 2 * CP_SIZE - 1
BLK = 128
LEAD = 2
MESH = pl.DeviceIdType.MESH
TURN = 2.0 ** 32
SIN_COEF = [(-1) ** k * (2 * math.pi) ** (2 * k + 1) / math.factorial(2 * k + 1) for k in range(7)]


def turn_tables(toks):
    turns = ROPE_BASE ** (-np.arange(0, HEAD_DIM, 2, dtype=np.float64) / HEAD_DIM) / (2 * math.pi)
    high = np.floor(turns * TURN)
    low = turns - high / TURN
    sub = 8
    lane_row = lax.broadcasted_iota(jnp.int32, (sub, toks), 0)
    parts = ([], [])
    for a in range(0, HALF_DIM, sub):
        for part, values, kind, num in zip(parts, (high, low), (jnp.int32, jnp.float32), (int, float)):
            tile = jnp.full((sub, toks), num(values[a]), kind)
            for c in range(1, sub):
                tile = jnp.where(lane_row == c, jnp.full((sub, toks), num(values[a + c]), kind), tile)
            part.append(tile)
    return [jnp.concatenate(part, axis=0) for part in parts]


def sin_turns(part):
    square = part * part
    total = jnp.full_like(part, SIN_COEF[-1])
    for coef in SIN_COEF[-2::-1]:
        total = total * square + coef
    return total * part


def nt_dot(lhs, rhs):
    return lax.dot_general(lhs, rhs, (((1,), (1,)), ((), ())), preferred_element_type=jnp.float32)


def rope_head(head, cos_tab, sin_tab):
    wide = head.astype(jnp.float32)
    return (wide * cos_tab + pltpu.roll(wide, HALF_DIM, 1) * sin_tab).astype(jnp.bfloat16)


def attend(kv_row, row_of, q_row, o_row, sb, group, dev, groups, fill):
    wide = (BLK, 2 * BLK)
    tri = lax.broadcasted_iota(jnp.int32, wide, 0) <= lax.rem(lax.broadcasted_iota(jnp.int32, wide, 1), BLK)
    units = [(half, g, h) for half in (1, 0) for g in groups for h in range(g * group, (g + 1) * group, 2)]

    def spans(half):
        n_blk = LAST - dev + 1 if half else dev + 1
        return n_blk, n_blk * BLK, slice(half * BLK, (half + 1) * BLK)

    starts, at = [], 0
    for half, _, _ in units:
        need = spans(half)[1]
        at = 0 if at + need > sb.shape[0] else at
        starts.append(at)
        at += need

    def score(k):
        half, g, h = units[k]
        n_blk, n_key, toks_at = spans(half)
        base = starts[k]
        keys = kv_row[0:n_blk, row_of(g):row_of(g) + BLK, :].reshape(n_key, HEAD_DIM)
        scores = nt_dot(keys, q_row[h:h + 2, toks_at, :].reshape(2 * BLK, HEAD_DIM))
        diag = jnp.where(tri, scores[n_key - BLK:], MASK_FILL)
        sb[base + n_key - BLK:base + n_key, :] = diag
        top = jnp.max(diag, axis=0, keepdims=True)
        if n_blk > 1:
            sb[base:base + n_key - BLK, :] = scores[:n_key - BLK]
            top = jnp.maximum(top, jnp.max(scores[:n_key - BLK], axis=0, keepdims=True))
        return top

    def weigh(k, top):
        half, g, h = units[k]
        n_blk, n_key, toks_at = spans(half)
        exp_w = jnp.exp2((sb[starts[k]:starts[k] + n_key, :] - top) * EXP_SCALE)
        inv = 1.0 / jnp.sum(exp_w, axis=0, keepdims=True)
        lo = row_of(g) + BLK
        vals = jnp.concatenate([kv_row[i, lo:lo + HEAD_DIM, :] for i in range(n_blk)], axis=1)
        out = (jnp.dot(vals, exp_w.astype(jnp.bfloat16), preferred_element_type=jnp.float32) * inv).T.astype(jnp.bfloat16)
        for i in range(2):
            o_row[toks_at, (h + i) * HEAD_DIM:(h + i + 1) * HEAD_DIM] = out[i * BLK:(i + 1) * BLK]

    count = len(units)
    tops = [score(k) for k in range(LEAD)]
    for k in range(count):
        if k + LEAD < count:
            tops.append(score(k + LEAD))
        weigh(k, tops[k])
        fill(k, count)


def main_kernel(x_hbm, pos_ref, wq_hbm, wk_hbm, wv_hbm, wo_hbm, xb, wo, kv_end, qb, ob,
                wq, wk, wv, kv, sb, high_b, low_b, cos_b, sin_b,
                xsem, wsem, ici_s, ici_r, sib_s, sib_r, fwd_s, fwd_r):
    rows, toks, width = xb.shape
    kv_cols = wk.shape[1]
    kv_heads = kv_cols // HEAD_DIM
    q_heads = wq.shape[1] // HEAD_DIM
    group = q_heads // kv_heads
    end = rows - 1
    me = lax.axis_index("cp")
    chip = me // 2
    core = lax.rem(me, 2)
    sib = chip * 2 + (1 - core)
    par = (1 - chip) * 2 + core
    dia = (1 - chip) * 2 + (1 - core)

    w_copies = [pltpu.make_async_copy(src, dst, wsem.at[i]) for i, (src, dst) in enumerate(((wk_hbm, wk), (wv_hbm, wv), (wq_hbm, wq), (wo_hbm, wo)))]

    def x_copy(b):
        return pltpu.make_async_copy(x_hbm.at[b], xb.at[b], xsem.at[b])

    def w_piece(src, dst, i, at, count):
        depth = src.shape[0] // count
        part = pl.ds(pl.multiple_of(at * depth, depth), depth)
        return pltpu.make_async_copy(src.at[part], dst.at[part], wsem.at[i])

    w_copies[0].start()
    x_copy(0).start()
    w_copies[1].start()
    high_b[...], low_b[...] = turn_tables(toks)

    barrier = pltpu.get_barrier_semaphore()
    for other in (sib, par):
        pl.semaphore_signal(barrier, inc=1, device_id={"cp": other}, device_id_type=MESH)
    pl.semaphore_wait(barrier, 2)

    def row_at(g):
        return g * (BLK + HEAD_DIM)

    def remote(b, idx, half, send, recv, dev, head=None):
        ref = kv.at[b, idx] if head is None else kv.at[b, idx, row_at(head):row_at(head + 1)]
        sem = b if head is None else b + head
        return pltpu.make_async_remote_copy(src_ref=ref, dst_ref=ref, send_sem=send.at[half, sem], recv_sem=recv.at[half, sem], device_id={"cp": dev}, device_id_type=MESH)

    def send_link(b, head=None):
        remote(b, me, 0, ici_s, ici_r, par, head).start()

        @pl.when(chip == 1)
        def _():
            remote(b, LAST - me, 1, ici_s, ici_r, par, head).start()

    def send_sib(b):
        remote(b, me, 0, sib_s, sib_r, sib).start()

        @pl.when(core == 1)
        def _():
            remote(b, LAST - me, 1, sib_s, sib_r, sib).start()

    def send_row(b):
        send_link(b)
        send_sib(b)

    def relay(b, head=None):
        remote(b, par, 0, ici_s, ici_r, par, head).wait_recv()
        remote(b, par, 0, fwd_s, fwd_r, sib, head).start()

        @pl.when(chip == 0)
        def _():
            remote(b, LAST - par, 1, ici_s, ici_r, par, head).wait_recv()
            remote(b, LAST - par, 1, fwd_s, fwd_r, sib, head).start()

    def wait_sib(b):
        remote(b, sib, 0, sib_s, sib_r, sib).wait_recv()

        @pl.when(core == 0)
        def _():
            remote(b, LAST - sib, 1, sib_s, sib_r, sib).wait_recv()

    def wait_relay(b, head=None):
        remote(b, dia, 0, fwd_s, fwd_r, sib, head).wait_recv()

        @pl.when(chip == 0)
        def _():
            remote(b, LAST - dia, 1, fwd_s, fwd_r, sib, head).wait_recv()

    def make_kv(b):
        pos = pos_ref[pl.ds(b, 1), :]
        turns = (pos * high_b[...]).astype(jnp.float32) * (1.0 / TURN) + pos.astype(jnp.float32) * low_b[...]
        turns = turns - jnp.round(turns)
        size = jnp.abs(turns)
        cosine = sin_turns(0.25 - size)
        sine = sin_turns(jnp.minimum(size, 0.5 - size))
        sine = jnp.where(turns < 0, -sine, sine)
        cos_tab = jnp.concatenate([cosine, cosine], axis=0).T
        sin_tab = jnp.concatenate([-sine, sine], axis=0).T
        cos_b[b] = cos_tab
        sin_b[b] = sin_tab
        x_row = xb[b]
        k_row = jnp.dot(x_row, wk[...], preferred_element_type=jnp.float32).astype(jnp.bfloat16)
        v_row = jnp.dot(x_row, wv[...], preferred_element_type=jnp.float32)
        for half, idx in ((0, me), (1, LAST - me)):
            lo = half * BLK
            for g in range(kv_heads):
                cols = slice(g * HEAD_DIM, (g + 1) * HEAD_DIM)
                at = row_at(g)
                kv[b, idx, at:at + BLK, :] = rope_head(k_row[lo:lo + BLK, cols], cos_tab[lo:lo + BLK], sin_tab[lo:lo + BLK])
                kv[b, idx, at + BLK:at + BLK + HEAD_DIM, :] = v_row[lo:lo + BLK, cols].T.astype(jnp.bfloat16)

    def make_q(b, slot):
        x_row = xb[b]
        cos_tab, sin_tab = cos_b[b], sin_b[b]
        for n in range(0, q_heads, 2):
            pair = jnp.dot(x_row, wq[:, n * HEAD_DIM:(n + 2) * HEAD_DIM], preferred_element_type=jnp.float32).astype(jnp.bfloat16)
            for i in range(2):
                qb[slot, n + i] = rope_head(pair[:, i * HEAD_DIM:(i + 1) * HEAD_DIM], cos_tab, sin_tab)

    out_tiles = width // (2 * HEAD_DIM)

    def out_tile(b, slot, n, keep):
        cols = slice(n * 2 * HEAD_DIM, (n + 1) * 2 * HEAD_DIM)
        y_part = jnp.dot(ob[slot], wo[:, cols], preferred_element_type=jnp.float32)
        if keep is not None:
            y_part = jnp.where(keep, y_part, 0.0)
        xb[b, :, cols] = (xb[b, :, cols].astype(jnp.float32) + y_part).astype(jnp.bfloat16)

    for b in range(1, 5):
        x_copy(b).start()
    w_copies[0].wait()
    x_copy(0).wait()
    w_copies[1].wait()
    make_kv(0)

    def kv_step(i, _):
        at = 2 * i + 1
        x_copy(at).wait()
        x_copy(at + 1).wait()

        @pl.when(i > 0)
        def _():
            send_row(at - 2)

        send_row(at - 1)
        for b in (at + 4, at + 5):
            @pl.when(b < rows)
            def _():
                x_copy(b).start()

        @pl.when(i < 3)
        def _():
            w_piece(wq_hbm, wq, 2, i, 3).start()

        @pl.when(i >= 3)
        def _():
            w_piece(wo_hbm, wo, 3, i - 3, 4).start()

        make_kv(at)
        make_kv(at + 1)
        return _

    lax.fori_loop(0, (rows - 2) // 2, kv_step, None)
    send_row(end - 2)
    send_row(end - 1)
    x_copy(end).wait()
    w_copies[2].wait()
    make_kv(end)
    make_q(0, 0)
    send_link(end, 0)
    send_link(end, 1)
    send_sib(end)
    w_copies[3].wait()

    def row_step(b, _):
        slot = lax.rem(b, 2)
        relay(b)
        make_q(b + 1, 1 - slot)
        wait_sib(b)
        wait_relay(b)

        def fill(k, count):
            if (k + 1) * out_tiles // count > k * out_tiles // count:
                out_tile(jnp.maximum(b - 1, 0), 1 - slot, k * out_tiles // count, b > 0)

        for dev in range(CP_SIZE):
            @pl.when(me == dev)
            def _():
                attend(kv.at[b], row_at, qb.at[slot], ob.at[slot], sb, group, dev, range(kv_heads), fill)

        return _

    lax.fori_loop(0, end, row_step, None)
    slot = end % 2
    relay(end, 0)
    for n in range(out_tiles):
        out_tile(end - 1, 1 - slot, n, None)
    wait_sib(end)
    wait_relay(end, 0)
    for dev in range(CP_SIZE):
        @pl.when(me == dev)
        def _():
            attend(kv.at[end], row_at, qb.at[slot], ob.at[slot], sb, group, dev, range(kv_heads - 1), lambda k, count: None)

    relay(end, 1)
    wait_relay(end, 1)
    kv_end[...] = kv[end, :, row_at(kv_heads - 1):row_at(kv_heads), :]

    def drain(b, head):
        remote(b, me, 0, ici_s, ici_r, par, head).wait_send()
        remote(b, par, 0, fwd_s, fwd_r, sib, head).wait_send()

        @pl.when(chip == 1)
        def _():
            remote(b, LAST - me, 1, ici_s, ici_r, par, head).wait_send()

        @pl.when(chip == 0)
        def _():
            remote(b, LAST - par, 1, fwd_s, fwd_r, sib, head).wait_send()

    def drain_sib(b):
        remote(b, me, 0, sib_s, sib_r, sib).wait_send()

        @pl.when(core == 1)
        def _():
            remote(b, LAST - me, 1, sib_s, sib_r, sib).wait_send()

    def drain_row(b, _):
        drain(b, None)
        drain_sib(b)
        return _

    lax.fori_loop(0, end, drain_row, None)
    drain(end, 0)
    drain(end, 1)
    drain_sib(end)


def end_kernel(xb, wo, kv_end, qb, ob, y_hbm, sb, o_new, acc, y_row, sem):
    rows, toks, width = xb.shape
    q_heads = qb.shape[1]
    kv_heads = 2
    group = q_heads // kv_heads
    end = rows - 1
    slot = end % 2
    me = lax.axis_index("cp")
    copies = [pltpu.make_async_copy(xb.at[b], y_hbm.at[b], sem.at[b]) for b in range(end)]
    for copy in copies:
        copy.start()
    old = (kv_heads - 1) * group * HEAD_DIM
    tile = 2 * HEAD_DIM
    out_tiles = width // tile

    def fill(k, count):
        for n in range(k * out_tiles // count, (k + 1) * out_tiles // count):
            cols = slice(n * tile, (n + 1) * tile)
            acc[:, cols] = xb[end, :, cols].astype(jnp.float32) + jnp.dot(ob[slot, :, :old], wo[:old, cols], preferred_element_type=jnp.float32)

    for dev in range(CP_SIZE):
        @pl.when(me == dev)
        def _():
            attend(kv_end, lambda g: 0, qb.at[slot], o_new, sb, group, dev, (kv_heads - 1,), fill)

    last_copies = []
    for n in range(out_tiles):
        cols = slice(n * tile, (n + 1) * tile)
        y_row[:, cols] = (acc[:, cols] + jnp.dot(o_new[:, old:], wo[old:, cols], preferred_element_type=jnp.float32)).astype(jnp.bfloat16)
        if n % 2:
            span = slice((n - 1) * tile, (n + 1) * tile)
            last_copies.append(pltpu.make_async_copy(y_row.at[:, span], y_hbm.at[end, :, span], sem.at[end + n // 2]))
            last_copies[-1].start()
    for copy in copies + last_copies:
        copy.wait()


def solution(mesh):
    row_spec = P('data', 'cp', None)
    pos_spec = P('data', 'cp')
    rep_spec = P(None, None)

    def local_block(x_loc, pos_loc, w_query, w_key, w_value, w_out):
        rows, toks, width = x_loc.shape
        q_cols, kv_cols = w_query.shape[1], w_key.shape[1]
        q_heads = q_cols // HEAD_DIM
        any_spec = pl.BlockSpec(memory_space=pl.ANY)
        vmem_spec = pl.BlockSpec(memory_space=pltpu.VMEM)
        bf16, f32 = jnp.bfloat16, jnp.float32
        pair_sem = pltpu.SemaphoreType.DMA((2, rows + 1))
        row_sem = pltpu.SemaphoreType.DMA((rows,))
        kept = pl.pallas_call(
            main_kernel,
            out_shape=[
                pltpu.VMEM(x_loc.shape, bf16),
                pltpu.VMEM((q_cols, width), bf16),
                pltpu.VMEM((2 * CP_SIZE, BLK + HEAD_DIM, BLK), bf16),
                pltpu.VMEM((2, q_heads, toks, HEAD_DIM), bf16),
                pltpu.VMEM((2, toks, q_cols), bf16),
            ],
            in_specs=[any_spec, vmem_spec] + [any_spec] * 4,
            out_specs=[vmem_spec] * 5,
            scratch_shapes=[
                pltpu.VMEM((width, q_cols), bf16),
                pltpu.VMEM((width, kv_cols), bf16),
                pltpu.VMEM((width, kv_cols), bf16),
                pltpu.VMEM((rows, 2 * CP_SIZE, 2 * kv_cols, BLK), bf16),
                pltpu.VMEM((4 * CP_SIZE * toks, 2 * BLK), f32),
                pltpu.VMEM((HALF_DIM, toks), jnp.int32),
                pltpu.VMEM((HALF_DIM, toks), f32),
                pltpu.VMEM((rows, toks, HEAD_DIM), f32),
                pltpu.VMEM((rows, toks, HEAD_DIM), f32),
                row_sem, pltpu.SemaphoreType.DMA((4,)),
                pair_sem, pair_sem, pair_sem, pair_sem, pair_sem, pair_sem,
            ],
            compiler_params=pltpu.CompilerParams(collective_id=0, has_side_effects=True, vmem_limit_bytes=36 * 1024 * 1024),
        )(x_loc, pos_loc, w_query, w_key, w_value, w_out)
        return pl.pallas_call(
            end_kernel,
            out_shape=jax.ShapeDtypeStruct(x_loc.shape, bf16),
            in_specs=[vmem_spec] * 5,
            out_specs=any_spec,
            scratch_shapes=[
                pltpu.VMEM((4 * CP_SIZE * toks, 2 * BLK), f32),
                pltpu.VMEM((toks, q_cols), bf16),
                pltpu.VMEM((toks, width), f32),
                pltpu.VMEM((toks, width), bf16),
                pltpu.SemaphoreType.DMA((rows + 2,)),
            ],
            compiler_params=pltpu.CompilerParams(vmem_limit_bytes=16 * 1024 * 1024),
        )(*kept)

    return jax.shard_map(local_block, mesh=mesh, in_specs=(row_spec, pos_spec, rep_spec, rep_spec, rep_spec, rep_spec), out_specs=row_spec, check_vma=False)
```

```python
import math

import jax
import jax.numpy as jnp
import numpy as np
from jax import lax
from jax.experimental import pallas as pl
from jax.experimental.pallas import tpu as pltpu
from jax.sharding import PartitionSpec as P

HEAD_DIM = 128
HALF_DIM = HEAD_DIM // 2
ROPE_BASE = 500000
MASK_FILL = -1e30
EXP_SCALE = math.log2(math.e) * HEAD_DIM ** -0.5
CP_SIZE = 4
LAST = 2 * CP_SIZE - 1
BLK = 128
LEAD = 3
MESH = pl.DeviceIdType.MESH
TURN = 2.0 ** 32
SIN_COEF = [(-1) ** k * (2 * math.pi) ** (2 * k + 1) / math.factorial(2 * k + 1) for k in range(7)]


def turn_tables(toks):
    turns = ROPE_BASE ** (-np.arange(0, HEAD_DIM, 2, dtype=np.float64) / HEAD_DIM) / (2 * math.pi)
    high = np.floor(turns * TURN)
    low = turns - high / TURN
    sub = 8
    lane_row = lax.broadcasted_iota(jnp.int32, (sub, toks), 0)
    parts = ([], [])
    for a in range(0, HALF_DIM, sub):
        for part, values, kind, num in zip(parts, (high, low), (jnp.int32, jnp.float32), (int, float)):
            tile = jnp.full((sub, toks), num(values[a]), kind)
            for c in range(1, sub):
                tile = jnp.where(lane_row == c, jnp.full((sub, toks), num(values[a + c]), kind), tile)
            part.append(tile)
    return [jnp.concatenate(part, axis=0) for part in parts]


def sin_turns(part):
    square = part * part
    total = jnp.full_like(part, SIN_COEF[-1])
    for coef in SIN_COEF[-2::-1]:
        total = total * square + coef
    return total * part


def nt_dot(lhs, rhs):
    return lax.dot_general(lhs, rhs, (((1,), (1,)), ((), ())), preferred_element_type=jnp.float32)


def rope_head(head, cos_tab, sin_tab):
    wide = head.astype(jnp.float32)
    return (wide * cos_tab + pltpu.roll(wide, HALF_DIM, 1) * sin_tab).astype(jnp.bfloat16)


def attend(kv_row, row_of, q_row, o_row, o_col, sb, dev, fill):
    wide = (BLK, 2 * BLK)
    tri = lax.broadcasted_iota(jnp.int32, wide, 0) <= lax.rem(lax.broadcasted_iota(jnp.int32, wide, 1), BLK)
    units = [(half, h) for half in (1, 0) for h in range(0, q_row.shape[0], 2)]

    def spans(half):
        n_blk = LAST - dev + 1 if half else dev + 1
        return n_blk, n_blk * BLK, slice(half * BLK, (half + 1) * BLK)

    starts, at = [], 0
    for half, _ in units:
        need = spans(half)[1]
        at = 0 if at + need > sb.shape[0] else at
        starts.append(at)
        at += need

    def score(k):
        half, h = units[k]
        n_blk, n_key, toks_at = spans(half)
        base = starts[k]
        keys = kv_row[0:n_blk, row_of:row_of + BLK, :].reshape(n_key, HEAD_DIM)
        scores = nt_dot(keys, q_row[h:h + 2, toks_at, :].reshape(2 * BLK, HEAD_DIM))
        diag = jnp.where(tri, scores[n_key - BLK:], MASK_FILL)
        sb[base + n_key - BLK:base + n_key, :] = diag
        top = jnp.max(diag, axis=0, keepdims=True)
        if n_blk > 1:
            sb[base:base + n_key - BLK, :] = scores[:n_key - BLK]
            top = jnp.maximum(top, jnp.max(scores[:n_key - BLK], axis=0, keepdims=True))
        return top

    def weigh(k, top):
        half, h = units[k]
        n_blk, n_key, toks_at = spans(half)
        exp_w = jnp.exp2((sb[starts[k]:starts[k] + n_key, :] - top) * EXP_SCALE)
        inv = 1.0 / jnp.sum(exp_w, axis=0, keepdims=True)
        lo = row_of + BLK
        vals = jnp.concatenate([kv_row[i, lo:lo + HEAD_DIM, :] for i in range(n_blk)], axis=1)
        out = (jnp.dot(vals, exp_w.astype(jnp.bfloat16), preferred_element_type=jnp.float32) * inv).T.astype(jnp.bfloat16)
        for i in range(2):
            o_row[toks_at, o_col + (h + i) * HEAD_DIM:o_col + (h + i + 1) * HEAD_DIM] = out[i * BLK:(i + 1) * BLK]

    count = len(units)
    tops = [score(k) for k in range(LEAD)]
    for k in range(count):
        if k + LEAD < count:
            tops.append(score(k + LEAD))
        weigh(k, tops[k])
        fill(k, count)


def main_kernel(x_hbm, pos_ref, wq_hbm, wk_hbm, wv_hbm, wo_hbm, xb, wo, kv_end, q_tail, o_head,
                wq, wk, wv, kv, q_head, q_next, o_full, sb, high_b, low_b, cos_b, sin_b,
                xsem, wsem, ici_s, ici_r, sib_s, sib_r, fwd_s, fwd_r):
    rows, toks, width = xb.shape
    kv_cols = wk.shape[1]
    kv_heads = kv_cols // HEAD_DIM
    q_heads = wq.shape[1] // HEAD_DIM
    group = q_heads // kv_heads
    head_cols = group * HEAD_DIM
    end = rows - 1
    me = lax.axis_index("cp")
    chip = me // 2
    core = lax.rem(me, 2)
    sib = chip * 2 + (1 - core)
    par = (1 - chip) * 2 + core
    dia = (1 - chip) * 2 + (1 - core)

    w_copies = [pltpu.make_async_copy(src, dst, wsem.at[i]) for i, (src, dst) in enumerate(((wk_hbm, wk), (wv_hbm, wv), (wq_hbm, wq), (wo_hbm, wo)))]

    def x_copy(b):
        return pltpu.make_async_copy(x_hbm.at[b], xb.at[b], xsem.at[b])

    def w_piece(src, dst, i, at, count):
        depth = src.shape[0] // count
        part = pl.ds(pl.multiple_of(at * depth, depth), depth)
        return pltpu.make_async_copy(src.at[part], dst.at[part], wsem.at[i])

    w_copies[0].start()
    x_copy(0).start()
    w_copies[1].start()
    high_b[...], low_b[...] = turn_tables(toks)

    barrier = pltpu.get_barrier_semaphore()
    for other in (sib, par):
        pl.semaphore_signal(barrier, inc=1, device_id={"cp": other}, device_id_type=MESH)
    pl.semaphore_wait(barrier, 2)

    def row_at(g):
        return g * (BLK + HEAD_DIM)

    def remote(b, idx, half, send, recv, dev, head):
        ref = kv.at[b, idx, row_at(head):row_at(head + 1)]
        return pltpu.make_async_remote_copy(src_ref=ref, dst_ref=ref, send_sem=send.at[half, head, b], recv_sem=recv.at[half, head, b], device_id={"cp": dev}, device_id_type=MESH)

    def sib_copy(b, idx, half):
        ref = kv.at[b, idx]
        return pltpu.make_async_remote_copy(src_ref=ref, dst_ref=ref, send_sem=sib_s.at[half, b], recv_sem=sib_r.at[half, b], device_id={"cp": sib}, device_id_type=MESH)

    def send_row(b):
        for head in range(kv_heads):
            remote(b, me, 0, ici_s, ici_r, par, head).start()

            @pl.when(chip == 1)
            def _():
                remote(b, LAST - me, 1, ici_s, ici_r, par, head).start()

        sib_copy(b, me, 0).start()

        @pl.when(core == 1)
        def _():
            sib_copy(b, LAST - me, 1).start()

    def relay(b, head):
        remote(b, par, 0, ici_s, ici_r, par, head).wait_recv()
        remote(b, par, 0, fwd_s, fwd_r, sib, head).start()

        @pl.when(chip == 0)
        def _():
            remote(b, LAST - par, 1, ici_s, ici_r, par, head).wait_recv()
            remote(b, LAST - par, 1, fwd_s, fwd_r, sib, head).start()

    def wait_sib(b):
        sib_copy(b, sib, 0).wait_recv()

        @pl.when(core == 0)
        def _():
            sib_copy(b, LAST - sib, 1).wait_recv()

    def wait_relay(b, head):
        remote(b, dia, 0, fwd_s, fwd_r, sib, head).wait_recv()

        @pl.when(chip == 0)
        def _():
            remote(b, LAST - dia, 1, fwd_s, fwd_r, sib, head).wait_recv()

    def make_kv(b):
        pos = pos_ref[pl.ds(b, 1), :]
        turns = (pos * high_b[...]).astype(jnp.float32) * (1.0 / TURN) + pos.astype(jnp.float32) * low_b[...]
        turns = turns - jnp.round(turns)
        size = jnp.abs(turns)
        cosine = sin_turns(0.25 - size)
        sine = sin_turns(jnp.minimum(size, 0.5 - size))
        sine = jnp.where(turns < 0, -sine, sine)
        cos_tab = jnp.concatenate([cosine, cosine], axis=0).T
        sin_tab = jnp.concatenate([-sine, sine], axis=0).T
        cos_b[b] = cos_tab
        sin_b[b] = sin_tab
        x_row = xb[b]
        k_row = jnp.dot(x_row, wk[...], preferred_element_type=jnp.float32).astype(jnp.bfloat16)
        v_row = jnp.dot(x_row, wv[...], preferred_element_type=jnp.float32)
        for half, idx in ((0, me), (1, LAST - me)):
            lo = half * BLK
            for g in range(kv_heads):
                cols = slice(g * HEAD_DIM, (g + 1) * HEAD_DIM)
                at = row_at(g)
                kv[b, idx, at:at + BLK, :] = rope_head(k_row[lo:lo + BLK, cols], cos_tab[lo:lo + BLK], sin_tab[lo:lo + BLK])
                kv[b, idx, at + BLK:at + BLK + HEAD_DIM, :] = v_row[lo:lo + BLK, cols].T.astype(jnp.bfloat16)

    def q_tile(b, n):
        cos_tab, sin_tab = cos_b[b], sin_b[b]
        pair = jnp.dot(xb[b], wq[:, n * HEAD_DIM:(n + 2) * HEAD_DIM], preferred_element_type=jnp.float32).astype(jnp.bfloat16)
        for i in range(2):
            ref, h = (q_head, n + i) if n < group else (q_next, n + i - group)
            ref[h] = rope_head(pair[:, i * HEAD_DIM:(i + 1) * HEAD_DIM], cos_tab, sin_tab)

    out_tiles = width // (2 * HEAD_DIM)

    def out_tile(b, n, keep):
        cols = slice(n * 2 * HEAD_DIM, (n + 1) * 2 * HEAD_DIM)
        y_part = jnp.where(keep, jnp.dot(o_full[...], wo[:, cols], preferred_element_type=jnp.float32), 0.0)
        xb[b, :, cols] = (xb[b, :, cols].astype(jnp.float32) + y_part).astype(jnp.bfloat16)

    for b in range(1, 5):
        x_copy(b).start()
    w_copies[0].wait()
    x_copy(0).wait()
    w_copies[1].wait()
    make_kv(0)

    def kv_step(i, _):
        at = 2 * i + 1
        x_copy(at).wait()
        x_copy(at + 1).wait()

        @pl.when(i > 0)
        def _():
            send_row(at - 2)

        send_row(at - 1)
        for b in (at + 4, at + 5):
            @pl.when(b < rows)
            def _():
                x_copy(b).start()

        @pl.when(i < 3)
        def _():
            w_piece(wq_hbm, wq, 2, i, 3).start()

        @pl.when(i >= 3)
        def _():
            w_piece(wo_hbm, wo, 3, i - 3, 4).start()

        make_kv(at)
        make_kv(at + 1)
        return _

    lax.fori_loop(0, (rows - 2) // 2, kv_step, None)
    send_row(end - 2)
    send_row(end - 1)
    x_copy(end).wait()
    w_copies[2].wait()
    make_kv(end)
    for n in range(0, q_heads, 2):
        q_tile(0, n)
    send_row(end)
    w_copies[3].wait()

    def spread(step, steps):
        def fill(k, count):
            for n in range(k * steps // count, (k + 1) * steps // count):
                step(n)
        return fill

    def row_step(b, _):
        b_old = jnp.maximum(b - 1, 0)
        relay(b, 0)

        @pl.when(b > 0)
        def _():
            wait_relay(b_old, 1)

        for dev in range(CP_SIZE):
            @pl.when((me == dev) & (b > 0))
            def _():
                o_full[:, :head_cols] = o_head[...]
                attend(kv.at[b_old], row_at(1), q_tail, o_full, head_cols, sb, dev, spread(lambda n: q_tile(b, 2 * n), q_heads // 2))

        wait_sib(b)
        wait_relay(b, 0)
        relay(b, 1)
        for dev in range(CP_SIZE):
            @pl.when(me == dev)
            def _():
                q_tail[...] = q_next[...]
                attend(kv.at[b], row_at(0), q_head, o_head, 0, sb, dev, spread(lambda n: out_tile(b_old, n, b > 0), out_tiles))

        return _

    lax.fori_loop(0, rows, row_step, None)
    wait_relay(end, 1)
    kv_end[...] = kv[end, :, row_at(kv_heads - 1):row_at(kv_heads), :]

    def drain_row(b, _):
        for head in range(kv_heads):
            remote(b, me, 0, ici_s, ici_r, par, head).wait_send()
            remote(b, par, 0, fwd_s, fwd_r, sib, head).wait_send()

            @pl.when(chip == 1)
            def _():
                remote(b, LAST - me, 1, ici_s, ici_r, par, head).wait_send()

            @pl.when(chip == 0)
            def _():
                remote(b, LAST - par, 1, fwd_s, fwd_r, sib, head).wait_send()

        sib_copy(b, me, 0).wait_send()

        @pl.when(core == 1)
        def _():
            sib_copy(b, LAST - me, 1).wait_send()

        return _

    lax.fori_loop(0, rows, drain_row, None)


def end_kernel(xb, wo, kv_end, q_tail, o_head, y_hbm, sb, o_tail, acc, y_row, sem):
    rows, toks, width = xb.shape
    end = rows - 1
    me = lax.axis_index("cp")
    copies = [pltpu.make_async_copy(xb.at[b], y_hbm.at[b], sem.at[b]) for b in range(end)]
    for copy in copies:
        copy.start()
    old = o_head.shape[1]
    tile = 2 * HEAD_DIM
    out_tiles = width // tile

    def fill(k, count):
        for n in range(k * out_tiles // count, (k + 1) * out_tiles // count):
            cols = slice(n * tile, (n + 1) * tile)
            acc[:, cols] = xb[end, :, cols].astype(jnp.float32) + jnp.dot(o_head[...], wo[:old, cols], preferred_element_type=jnp.float32)

    for dev in range(CP_SIZE):
        @pl.when(me == dev)
        def _():
            attend(kv_end, 0, q_tail, o_tail, 0, sb, dev, fill)

    last_copies = []
    for n in range(out_tiles):
        cols = slice(n * tile, (n + 1) * tile)
        y_row[:, cols] = (acc[:, cols] + jnp.dot(o_tail[...], wo[old:, cols], preferred_element_type=jnp.float32)).astype(jnp.bfloat16)
        if n % 2:
            span = slice((n - 1) * tile, (n + 1) * tile)
            last_copies.append(pltpu.make_async_copy(y_row.at[:, span], y_hbm.at[end, :, span], sem.at[end + n // 2]))
            last_copies[-1].start()
    for copy in copies + last_copies:
        copy.wait()


def solution(mesh):
    row_spec = P('data', 'cp', None)
    pos_spec = P('data', 'cp')
    rep_spec = P(None, None)

    def local_block(x_loc, pos_loc, w_query, w_key, w_value, w_out):
        rows, toks, width = x_loc.shape
        q_cols, kv_cols = w_query.shape[1], w_key.shape[1]
        group = q_cols // kv_cols
        any_spec = pl.BlockSpec(memory_space=pl.ANY)
        vmem_spec = pl.BlockSpec(memory_space=pltpu.VMEM)
        bf16, f32 = jnp.bfloat16, jnp.float32
        pair_sem = pltpu.SemaphoreType.DMA((2, rows))
        head_sem = pltpu.SemaphoreType.DMA((2, kv_cols // HEAD_DIM, rows))
        row_sem = pltpu.SemaphoreType.DMA((rows,))
        kept = pl.pallas_call(
            main_kernel,
            out_shape=[
                pltpu.VMEM(x_loc.shape, bf16),
                pltpu.VMEM((q_cols, width), bf16),
                pltpu.VMEM((2 * CP_SIZE, BLK + HEAD_DIM, BLK), bf16),
                pltpu.VMEM((group, toks, HEAD_DIM), bf16),
                pltpu.VMEM((toks, group * HEAD_DIM), bf16),
            ],
            in_specs=[any_spec, vmem_spec] + [any_spec] * 4,
            out_specs=[vmem_spec] * 5,
            scratch_shapes=[
                pltpu.VMEM((width, q_cols), bf16),
                pltpu.VMEM((width, kv_cols), bf16),
                pltpu.VMEM((width, kv_cols), bf16),
                pltpu.VMEM((rows, 2 * CP_SIZE, 2 * kv_cols, BLK), bf16),
                pltpu.VMEM((group, toks, HEAD_DIM), bf16),
                pltpu.VMEM((group, toks, HEAD_DIM), bf16),
                pltpu.VMEM((toks, q_cols), bf16),
                pltpu.VMEM((4 * CP_SIZE * toks, 2 * BLK), f32),
                pltpu.VMEM((HALF_DIM, toks), jnp.int32),
                pltpu.VMEM((HALF_DIM, toks), f32),
                pltpu.VMEM((rows, toks, HEAD_DIM), f32),
                pltpu.VMEM((rows, toks, HEAD_DIM), f32),
                row_sem, pltpu.SemaphoreType.DMA((4,)),
                head_sem, head_sem, pair_sem, pair_sem, head_sem, head_sem,
            ],
            compiler_params=pltpu.CompilerParams(collective_id=0, has_side_effects=True, vmem_limit_bytes=36 * 1024 * 1024),
        )(x_loc, pos_loc, w_query, w_key, w_value, w_out)
        return pl.pallas_call(
            end_kernel,
            out_shape=jax.ShapeDtypeStruct(x_loc.shape, bf16),
            in_specs=[vmem_spec] * 5,
            out_specs=any_spec,
            scratch_shapes=[
                pltpu.VMEM((4 * CP_SIZE * toks, 2 * BLK), f32),
                pltpu.VMEM((toks, group * HEAD_DIM), bf16),
                pltpu.VMEM((toks, width), f32),
                pltpu.VMEM((toks, width), bf16),
                pltpu.SemaphoreType.DMA((rows + 2,)),
            ],
            compiler_params=pltpu.CompilerParams(vmem_limit_bytes=16 * 1024 * 1024),
        )(*kept)

    return jax.shard_map(local_block, mesh=mesh, in_specs=(row_spec, pos_spec, rep_spec, rep_spec, rep_spec, rep_spec), out_specs=row_spec, check_vma=False)
```

```python
import math

import jax
import jax.numpy as jnp
import numpy as np
from jax import lax
from jax.experimental import pallas as pl
from jax.experimental.pallas import tpu as pltpu
from jax.sharding import PartitionSpec as P

HEAD_DIM = 128
HALF_DIM = HEAD_DIM // 2
ROPE_BASE = 500000
MASK_FILL = -1e30
EXP_SCALE = math.log2(math.e) * HEAD_DIM ** -0.5
CP_SIZE = 4
LAST = 2 * CP_SIZE - 1
BLK = 128
LEAD = 3
MESH = pl.DeviceIdType.MESH
TURN = 2.0 ** 32
SIN_COEF = [(-1) ** k * (2 * math.pi) ** (2 * k + 1) / math.factorial(2 * k + 1) for k in range(7)]


def turn_tables(toks):
    turns = ROPE_BASE ** (-np.arange(0, HEAD_DIM, 2, dtype=np.float64) / HEAD_DIM) / (2 * math.pi)
    high = np.floor(turns * TURN)
    low = turns - high / TURN
    sub = 8
    lane_row = lax.broadcasted_iota(jnp.int32, (sub, toks), 0)
    parts = ([], [])
    for a in range(0, HALF_DIM, sub):
        for part, values, kind, num in zip(parts, (high, low), (jnp.int32, jnp.float32), (int, float)):
            tile = jnp.full((sub, toks), num(values[a]), kind)
            for c in range(1, sub):
                tile = jnp.where(lane_row == c, jnp.full((sub, toks), num(values[a + c]), kind), tile)
            part.append(tile)
    return [jnp.concatenate(part, axis=0) for part in parts]


def sin_turns(part):
    square = part * part
    total = jnp.full_like(part, SIN_COEF[-1])
    for coef in SIN_COEF[-2::-1]:
        total = total * square + coef
    return total * part


def nt_dot(lhs, rhs):
    return lax.dot_general(lhs, rhs, (((1,), (1,)), ((), ())), preferred_element_type=jnp.float32)


def rope_head(head, cos_tab, sin_tab):
    wide = head.astype(jnp.float32)
    return (wide * cos_tab + pltpu.roll(wide, HALF_DIM, 1) * sin_tab).astype(jnp.bfloat16)


def attend(kv_row, row_of, q_row, o_row, o_col, sb, dev, fill):
    wide = (BLK, 2 * BLK)
    tri = lax.broadcasted_iota(jnp.int32, wide, 0) <= lax.rem(lax.broadcasted_iota(jnp.int32, wide, 1), BLK)
    units = [(half, h) for half in (1, 0) for h in range(0, q_row.shape[0], 2)]

    def spans(half):
        n_blk = LAST - dev + 1 if half else dev + 1
        return n_blk, n_blk * BLK, slice(half * BLK, (half + 1) * BLK)

    starts, at = [], 0
    for half, _ in units:
        need = spans(half)[1]
        at = 0 if at + need > sb.shape[0] else at
        starts.append(at)
        at += need

    def score(k):
        half, h = units[k]
        n_blk, n_key, toks_at = spans(half)
        base = starts[k]
        keys = kv_row[0:n_blk, row_of:row_of + BLK, :].reshape(n_key, HEAD_DIM)
        scores = nt_dot(keys, q_row[h:h + 2, toks_at, :].reshape(2 * BLK, HEAD_DIM))
        diag = jnp.where(tri, scores[n_key - BLK:], MASK_FILL)
        sb[base + n_key - BLK:base + n_key, :] = diag
        top = jnp.max(diag, axis=0, keepdims=True)
        if n_blk > 1:
            sb[base:base + n_key - BLK, :] = scores[:n_key - BLK]
            top = jnp.maximum(top, jnp.max(scores[:n_key - BLK], axis=0, keepdims=True))
        return top

    def weigh(k, top):
        half, h = units[k]
        n_blk, n_key, toks_at = spans(half)
        exp_w = jnp.exp2((sb[starts[k]:starts[k] + n_key, :] - top) * EXP_SCALE)
        inv = 1.0 / jnp.sum(exp_w, axis=0, keepdims=True)
        lo = row_of + BLK
        vals = jnp.concatenate([kv_row[i, lo:lo + HEAD_DIM, :] for i in range(n_blk)], axis=1)
        out = (jnp.dot(vals, exp_w.astype(jnp.bfloat16), preferred_element_type=jnp.float32) * inv).T.astype(jnp.bfloat16)
        for i in range(2):
            o_row[toks_at, o_col + (h + i) * HEAD_DIM:o_col + (h + i + 1) * HEAD_DIM] = out[i * BLK:(i + 1) * BLK]

    count = len(units)
    tops = [score(k) for k in range(LEAD)]
    for k in range(count):
        if k + LEAD < count:
            tops.append(score(k + LEAD))
        weigh(k, tops[k])
        fill(k, count)


def main_kernel(x_hbm, pos_hbm, wq_hbm, wk_hbm, wv_hbm, wo_hbm, xb, wo, kv_end, q_tail, o_head,
                wq, wk, wv, kv, q_head, q_next, o_full, sb, pos_ref, high_b, low_b, cos_b, sin_b,
                xsem, wsem, ici_s, ici_r, sib_s, sib_r, fwd_s, fwd_r):
    rows, toks, width = xb.shape
    kv_cols = wk.shape[1]
    kv_heads = kv_cols // HEAD_DIM
    q_heads = wq.shape[1] // HEAD_DIM
    group = q_heads // kv_heads
    head_cols = group * HEAD_DIM
    end = rows - 1
    me = lax.axis_index("cp")
    chip = me // 2
    core = lax.rem(me, 2)
    sib = chip * 2 + (1 - core)
    par = (1 - chip) * 2 + core
    dia = (1 - chip) * 2 + (1 - core)

    w_copies = [pltpu.make_async_copy(src, dst, wsem.at[i]) for i, (src, dst) in enumerate(((wk_hbm, wk), (wv_hbm, wv), (wq_hbm, wq), (wo_hbm, wo), (pos_hbm, pos_ref)))]

    def x_copy(b):
        return pltpu.make_async_copy(x_hbm.at[b], xb.at[b], xsem.at[b])

    def w_piece(src, dst, i, at, count):
        depth = src.shape[0] // count
        part = pl.ds(pl.multiple_of(at * depth, depth), depth)
        return pltpu.make_async_copy(src.at[part], dst.at[part], wsem.at[i])

    w_copies[0].start()
    x_copy(0).start()
    w_copies[4].start()
    w_copies[1].start()
    barrier = pltpu.get_barrier_semaphore()
    for other in (sib, par):
        pl.semaphore_signal(barrier, inc=1, device_id={"cp": other}, device_id_type=MESH)
    high_b[...], low_b[...] = turn_tables(toks)

    def row_at(g):
        return g * (BLK + HEAD_DIM)

    def piece(b, idx, head):
        return kv.at[b, idx] if head is None else kv.at[b, idx, row_at(head):row_at(head + 1)]

    def remote(ref, send, recv, dev):
        return pltpu.make_async_remote_copy(src_ref=ref, dst_ref=ref, send_sem=send, recv_sem=recv, device_id={"cp": dev}, device_id_type=MESH)

    def either(twin, act):
        @pl.when(twin)
        def _():
            act(2)

        @pl.when(jnp.logical_not(twin))
        def _():
            act(1)

    def send_row(b):
        for head in range(kv_heads):
            remote(piece(b, me, head), ici_s, ici_r.at[head, b], par).start()

            @pl.when(chip == 1)
            def _():
                remote(piece(b, LAST - me, head), ici_s, ici_r.at[head, b], par).start()

        remote(piece(b, me, None), sib_s, sib_r.at[b], sib).start()

        @pl.when(core == 1)
        def _():
            remote(piece(b, LAST - me, None), sib_s, sib_r.at[b], sib).start()

    def relay(b, head):
        either(chip == 0, lambda n: remote(piece(b, slice(0, n), head), ici_s, ici_r.at[head, b], par).wait_recv())
        remote(piece(b, par, head), fwd_s, fwd_r.at[head, b], sib).start()

        @pl.when(chip == 0)
        def _():
            remote(piece(b, LAST - par, head), fwd_s, fwd_r.at[head, b], sib).start()

    def wait_sib(b):
        either(core == 0, lambda n: remote(piece(b, slice(0, n), None), sib_s, sib_r.at[b], sib).wait_recv())

    def wait_relay(b, head):
        either(chip == 0, lambda n: remote(piece(b, slice(0, n), head), fwd_s, fwd_r.at[head, b], sib).wait_recv())

    def make_kv(b):
        pos = pos_ref[pl.ds(b, 1), :]
        turns = (pos * high_b[...]).astype(jnp.float32) * (1.0 / TURN) + pos.astype(jnp.float32) * low_b[...]
        turns = turns - jnp.round(turns)
        size = jnp.abs(turns)
        cosine = sin_turns(0.25 - size)
        sine = sin_turns(jnp.minimum(size, 0.5 - size))
        sine = jnp.where(turns < 0, -sine, sine)
        cos_tab = jnp.concatenate([cosine, cosine], axis=0).T
        sin_tab = jnp.concatenate([-sine, sine], axis=0).T
        cos_b[b] = cos_tab
        sin_b[b] = sin_tab
        x_row = xb[b]
        k_row = jnp.dot(x_row, wk[...], preferred_element_type=jnp.float32).astype(jnp.bfloat16)
        v_row = jnp.dot(x_row, wv[...], preferred_element_type=jnp.float32)
        for half, idx in ((0, me), (1, LAST - me)):
            lo = half * BLK
            for g in range(kv_heads):
                cols = slice(g * HEAD_DIM, (g + 1) * HEAD_DIM)
                at = row_at(g)
                kv[b, idx, at:at + BLK, :] = rope_head(k_row[lo:lo + BLK, cols], cos_tab[lo:lo + BLK], sin_tab[lo:lo + BLK])
                kv[b, idx, at + BLK:at + BLK + HEAD_DIM, :] = v_row[lo:lo + BLK, cols].T.astype(jnp.bfloat16)

    def q_tile(b, n):
        cos_tab, sin_tab = cos_b[b], sin_b[b]
        pair = jnp.dot(xb[b], wq[:, n * HEAD_DIM:(n + 2) * HEAD_DIM], preferred_element_type=jnp.float32).astype(jnp.bfloat16)
        for i in range(2):
            ref, h = (q_head, n + i) if n < group else (q_next, n + i - group)
            ref[h] = rope_head(pair[:, i * HEAD_DIM:(i + 1) * HEAD_DIM], cos_tab, sin_tab)

    out_tiles = width // (2 * HEAD_DIM)

    def out_tile(b, n, keep):
        cols = slice(n * 2 * HEAD_DIM, (n + 1) * 2 * HEAD_DIM)
        y_part = jnp.where(keep, jnp.dot(o_full[...], wo[:, cols], preferred_element_type=jnp.float32), 0.0)
        xb[b, :, cols] = (xb[b, :, cols].astype(jnp.float32) + y_part).astype(jnp.bfloat16)

    for copy in (w_copies[4], w_copies[0], x_copy(0)):
        copy.wait()
    for b in range(1, 5):
        x_copy(b).start()
    w_copies[1].wait()
    make_kv(0)
    pl.semaphore_wait(barrier, 2)
    send_row(0)

    def kv_step(i, _):
        at = 2 * i + 1
        x_copy(at).wait()
        x_copy(at + 1).wait()

        @pl.when(i > 0)
        def _():
            send_row(at - 2)
            send_row(at - 1)

        for b in (at + 4, at + 5):
            @pl.when(b < rows)
            def _():
                x_copy(b).start()

        @pl.when(i < 3)
        def _():
            w_piece(wq_hbm, wq, 2, i, 3).start()

        @pl.when(i >= 3)
        def _():
            w_piece(wo_hbm, wo, 3, i - 3, 4).start()

        make_kv(at)
        make_kv(at + 1)
        return _

    lax.fori_loop(0, (rows - 2) // 2, kv_step, None)
    send_row(end - 2)
    send_row(end - 1)
    x_copy(end).wait()
    w_copies[2].wait()
    make_kv(end)
    for n in range(0, q_heads, 2):
        q_tile(0, n)
    send_row(end)
    w_copies[3].wait()

    def spread(step, steps):
        def fill(k, count):
            for n in range(k * steps // count, (k + 1) * steps // count):
                step(n)
        return fill

    def row_step(b, _):
        b_old = jnp.maximum(b - 1, 0)
        relay(b, 0)

        @pl.when(b > 0)
        def _():
            wait_relay(b_old, 1)

        for dev in range(CP_SIZE):
            @pl.when((me == dev) & (b > 0))
            def _():
                o_full[:, :head_cols] = o_head[...]
                attend(kv.at[b_old], row_at(1), q_tail, o_full, head_cols, sb, dev, spread(lambda n: q_tile(b, 2 * n), q_heads // 2))

        wait_sib(b)
        wait_relay(b, 0)
        relay(b, 1)
        for dev in range(CP_SIZE):
            @pl.when(me == dev)
            def _():
                q_tail[...] = q_next[...]
                attend(kv.at[b], row_at(0), q_head, o_head, 0, sb, dev, spread(lambda n: out_tile(b_old, n, b > 0), out_tiles))

        return _

    lax.fori_loop(0, rows, row_step, None)
    wait_relay(end, 1)
    kv_end[...] = kv[end, :, row_at(kv_heads - 1):row_at(kv_heads), :]

    either(chip == 1, lambda n: remote(kv.at[:, 0:n], ici_s, ici_r.at[0, 0], par).wait_send())
    either(chip == 0, lambda n: remote(kv.at[:, 0:n], fwd_s, fwd_r.at[0, 0], sib).wait_send())
    either(core == 1, lambda n: remote(kv.at[:, 0:n], sib_s, sib_r.at[0], sib).wait_send())


def end_kernel(xb, wo, kv_end, q_tail, o_head, y_hbm, sb, o_tail, acc, y_row, sem):
    rows, toks, width = xb.shape
    end = rows - 1
    me = lax.axis_index("cp")
    copies = [pltpu.make_async_copy(xb.at[b], y_hbm.at[b], sem.at[b]) for b in range(end)]
    for copy in copies:
        copy.start()
    old = o_head.shape[1]
    tile = 2 * HEAD_DIM
    out_tiles = width // tile

    def fill(k, count):
        for n in range(k * out_tiles // count, (k + 1) * out_tiles // count):
            cols = slice(n * tile, (n + 1) * tile)
            acc[:, cols] = xb[end, :, cols].astype(jnp.float32) + jnp.dot(o_head[...], wo[:old, cols], preferred_element_type=jnp.float32)

    for dev in range(CP_SIZE):
        @pl.when(me == dev)
        def _():
            attend(kv_end, 0, q_tail, o_tail, 0, sb, dev, fill)

    last_copies = []
    for n in range(out_tiles):
        cols = slice(n * tile, (n + 1) * tile)
        y_row[:, cols] = (acc[:, cols] + jnp.dot(o_tail[...], wo[old:, cols], preferred_element_type=jnp.float32)).astype(jnp.bfloat16)
        if n % 2:
            span = slice((n - 1) * tile, (n + 1) * tile)
            last_copies.append(pltpu.make_async_copy(y_row.at[:, span], y_hbm.at[end, :, span], sem.at[end + n // 2]))
            last_copies[-1].start()
    for copy in copies + last_copies:
        copy.wait()


def solution(mesh):
    row_spec = P('data', 'cp', None)
    pos_spec = P('data', 'cp')
    rep_spec = P(None, None)

    def local_block(x_loc, pos_loc, w_query, w_key, w_value, w_out):
        rows, toks, width = x_loc.shape
        q_cols, kv_cols = w_query.shape[1], w_key.shape[1]
        group = q_cols // kv_cols
        any_spec = pl.BlockSpec(memory_space=pl.ANY)
        vmem_spec = pl.BlockSpec(memory_space=pltpu.VMEM)
        bf16, f32 = jnp.bfloat16, jnp.float32
        one_sem = pltpu.SemaphoreType.DMA
        head_sem = pltpu.SemaphoreType.DMA((kv_cols // HEAD_DIM, rows))
        row_sem = pltpu.SemaphoreType.DMA((rows,))
        kept = pl.pallas_call(
            main_kernel,
            out_shape=[
                pltpu.VMEM(x_loc.shape, bf16),
                pltpu.VMEM((q_cols, width), bf16),
                pltpu.VMEM((2 * CP_SIZE, BLK + HEAD_DIM, BLK), bf16),
                pltpu.VMEM((group, toks, HEAD_DIM), bf16),
                pltpu.VMEM((toks, group * HEAD_DIM), bf16),
            ],
            in_specs=[any_spec] * 6,
            out_specs=[vmem_spec] * 5,
            scratch_shapes=[
                pltpu.VMEM((width, q_cols), bf16),
                pltpu.VMEM((width, kv_cols), bf16),
                pltpu.VMEM((width, kv_cols), bf16),
                pltpu.VMEM((rows, 2 * CP_SIZE, 2 * kv_cols, BLK), bf16),
                pltpu.VMEM((group, toks, HEAD_DIM), bf16),
                pltpu.VMEM((group, toks, HEAD_DIM), bf16),
                pltpu.VMEM((toks, q_cols), bf16),
                pltpu.VMEM((4 * CP_SIZE * toks, 2 * BLK), f32),
                pltpu.VMEM((rows, toks), jnp.int32),
                pltpu.VMEM((HALF_DIM, toks), jnp.int32),
                pltpu.VMEM((HALF_DIM, toks), f32),
                pltpu.VMEM((rows, toks, HEAD_DIM), f32),
                pltpu.VMEM((rows, toks, HEAD_DIM), f32),
                row_sem, pltpu.SemaphoreType.DMA((5,)),
                one_sem, head_sem, one_sem, row_sem, one_sem, head_sem,
            ],
            compiler_params=pltpu.CompilerParams(collective_id=0, has_side_effects=True, vmem_limit_bytes=43 * 1024 * 1024),
        )(x_loc, pos_loc, w_query, w_key, w_value, w_out)
        return pl.pallas_call(
            end_kernel,
            out_shape=jax.ShapeDtypeStruct(x_loc.shape, bf16),
            in_specs=[vmem_spec] * 5,
            out_specs=any_spec,
            scratch_shapes=[
                pltpu.VMEM((4 * CP_SIZE * toks, 2 * BLK), f32),
                pltpu.VMEM((toks, group * HEAD_DIM), bf16),
                pltpu.VMEM((toks, width), f32),
                pltpu.VMEM((toks, width), bf16),
                pltpu.SemaphoreType.DMA((rows + 2,)),
            ],
            compiler_params=pltpu.CompilerParams(vmem_limit_bytes=16 * 1024 * 1024),
        )(*kept)

    return jax.shard_map(local_block, mesh=mesh, in_specs=(row_spec, pos_spec, rep_spec, rep_spec, rep_spec, rep_spec), out_specs=row_spec, check_vma=False)
```

```python
import math

import jax
import jax.numpy as jnp
import numpy as np
from jax import lax
from jax.experimental import pallas as pl
from jax.experimental.pallas import tpu as pltpu
from jax.sharding import PartitionSpec as P

HEAD_DIM = 128
HALF_DIM = HEAD_DIM // 2
ROPE_BASE = 500000
MASK_FILL = -1e30
EXP_SCALE = math.log2(math.e) * HEAD_DIM ** -0.5
CP_SIZE = 4
LAST = 2 * CP_SIZE - 1
BLK = 128
LEAD = 3
MESH = pl.DeviceIdType.MESH
TURN = 2.0 ** 32
SIN_COEF = [(-1) ** k * (2 * math.pi) ** (2 * k + 1) / math.factorial(2 * k + 1) for k in range(7)]


def turn_tables(toks):
    turns = ROPE_BASE ** (-np.arange(0, HEAD_DIM, 2, dtype=np.float64) / HEAD_DIM) / (2 * math.pi)
    high = np.floor(turns * TURN)
    low = turns - high / TURN
    sub = 8
    lane_row = lax.broadcasted_iota(jnp.int32, (sub, toks), 0)
    parts = ([], [])
    for a in range(0, HALF_DIM, sub):
        for part, values, kind, num in zip(parts, (high, low), (jnp.int32, jnp.float32), (int, float)):
            tile = jnp.full((sub, toks), num(values[a]), kind)
            for c in range(1, sub):
                tile = jnp.where(lane_row == c, jnp.full((sub, toks), num(values[a + c]), kind), tile)
            part.append(tile)
    return [jnp.concatenate(part, axis=0) for part in parts]


def sin_turns(part):
    square = part * part
    total = jnp.full_like(part, SIN_COEF[-1])
    for coef in SIN_COEF[-2::-1]:
        total = total * square + coef
    return total * part


def nt_dot(lhs, rhs):
    return lax.dot_general(lhs, rhs, (((1,), (1,)), ((), ())), preferred_element_type=jnp.float32)


def rope_head(head, cos_tab, sin_tab):
    wide = head.astype(jnp.float32)
    return (wide * cos_tab + pltpu.roll(wide, HALF_DIM, 1) * sin_tab).astype(jnp.bfloat16)


def attend(kv_row, row_of, q_row, o_row, o_col, sb, dev, fill):
    wide = (BLK, 2 * BLK)
    tri = lax.broadcasted_iota(jnp.int32, wide, 0) <= lax.rem(lax.broadcasted_iota(jnp.int32, wide, 1), BLK)
    units = [(half, h) for half in (1, 0) for h in range(0, q_row.shape[0], 2)]

    def spans(half):
        n_blk = LAST - dev + 1 if half else dev + 1
        return n_blk, n_blk * BLK, slice(half * BLK, (half + 1) * BLK)

    starts, at = [], 0
    for half, _ in units:
        need = spans(half)[1]
        at = 0 if at + need > sb.shape[0] else at
        starts.append(at)
        at += need

    def score(k):
        half, h = units[k]
        n_blk, n_key, toks_at = spans(half)
        base = starts[k]
        keys = kv_row[0:n_blk, row_of:row_of + BLK, :].reshape(n_key, HEAD_DIM)
        scores = nt_dot(keys, q_row[h:h + 2, toks_at, :].reshape(2 * BLK, HEAD_DIM))
        diag = jnp.where(tri, scores[n_key - BLK:], MASK_FILL)
        sb[base + n_key - BLK:base + n_key, :] = diag
        top = jnp.max(diag, axis=0, keepdims=True)
        if n_blk > 1:
            sb[base:base + n_key - BLK, :] = scores[:n_key - BLK]
            top = jnp.maximum(top, jnp.max(scores[:n_key - BLK], axis=0, keepdims=True))
        return top

    def weigh(k, top):
        half, h = units[k]
        n_blk, n_key, toks_at = spans(half)
        exp_w = jnp.exp2((sb[starts[k]:starts[k] + n_key, :] - top) * EXP_SCALE)
        inv = 1.0 / jnp.sum(exp_w, axis=0, keepdims=True)
        lo = row_of + BLK
        vals = jnp.concatenate([kv_row[i, lo:lo + HEAD_DIM, :] for i in range(n_blk)], axis=1)
        out = (jnp.dot(vals, exp_w.astype(jnp.bfloat16), preferred_element_type=jnp.float32) * inv).T.astype(jnp.bfloat16)
        for i in range(2):
            o_row[toks_at, o_col + (h + i) * HEAD_DIM:o_col + (h + i + 1) * HEAD_DIM] = out[i * BLK:(i + 1) * BLK]

    count = len(units)
    tops = [score(k) for k in range(LEAD)]
    for k in range(count):
        if k + LEAD < count:
            tops.append(score(k + LEAD))
        weigh(k, tops[k])
        fill(k, count)


def main_kernel(x_hbm, pos_hbm, wq_hbm, wk_hbm, wv_hbm, wo_hbm, xb, wo, kv_end, q_head, q_next, o_full,
                wq, wk, wv, kv, q_tail, o_head, sb, pos_ref, high_b, low_b, cos_b, sin_b,
                xsem, wsem, ici_s, ici_r, sib_s, sib_r, fwd_s, fwd_r):
    rows, toks, width = xb.shape
    kv_cols = wk.shape[1]
    kv_heads = kv_cols // HEAD_DIM
    q_heads = wq.shape[1] // HEAD_DIM
    group = q_heads // kv_heads
    head_cols = group * HEAD_DIM
    end = rows - 1
    me = lax.axis_index("cp")
    chip = me // 2
    core = lax.rem(me, 2)
    sib = chip * 2 + (1 - core)
    par = (1 - chip) * 2 + core
    dia = (1 - chip) * 2 + (1 - core)

    w_copies = [pltpu.make_async_copy(src, dst, wsem.at[i]) for i, (src, dst) in enumerate(((wk_hbm, wk), (wv_hbm, wv), (wq_hbm, wq), (wo_hbm, wo), (pos_hbm, pos_ref)))]

    def x_copy(b):
        return pltpu.make_async_copy(x_hbm.at[b], xb.at[b], xsem.at[b])

    def w_piece(src, dst, i, at, count):
        depth = src.shape[0] // count
        part = pl.ds(pl.multiple_of(at * depth, depth), depth)
        return pltpu.make_async_copy(src.at[part], dst.at[part], wsem.at[i])

    w_copies[0].start()
    x_copy(0).start()
    w_copies[4].start()
    w_copies[1].start()
    barrier = pltpu.get_barrier_semaphore()
    for other in (sib, par):
        pl.semaphore_signal(barrier, inc=1, device_id={"cp": other}, device_id_type=MESH)
    high_b[...], low_b[...] = turn_tables(toks)

    def row_at(g):
        return g * (BLK + HEAD_DIM)

    def piece(b, idx, head):
        return kv.at[b, idx] if head is None else kv.at[b, idx, row_at(head):row_at(head + 1)]

    def remote(ref, send, recv, dev):
        return pltpu.make_async_remote_copy(src_ref=ref, dst_ref=ref, send_sem=send, recv_sem=recv, device_id={"cp": dev}, device_id_type=MESH)

    def either(twin, act):
        @pl.when(twin)
        def _():
            act(2)

        @pl.when(jnp.logical_not(twin))
        def _():
            act(1)

    def send_row(b):
        for head in range(kv_heads):
            remote(piece(b, me, head), ici_s, ici_r.at[head, b], par).start()

            @pl.when(chip == 1)
            def _():
                remote(piece(b, LAST - me, head), ici_s, ici_r.at[head, b], par).start()

        remote(piece(b, me, None), sib_s, sib_r.at[b], sib).start()

        @pl.when(core == 1)
        def _():
            remote(piece(b, LAST - me, None), sib_s, sib_r.at[b], sib).start()

    def relay(b, head):
        either(chip == 0, lambda n: remote(piece(b, slice(0, n), head), ici_s, ici_r.at[head, b], par).wait_recv())
        remote(piece(b, par, head), fwd_s, fwd_r.at[head, b], sib).start()

        @pl.when(chip == 0)
        def _():
            remote(piece(b, LAST - par, head), fwd_s, fwd_r.at[head, b], sib).start()

    def wait_sib(b):
        either(core == 0, lambda n: remote(piece(b, slice(0, n), None), sib_s, sib_r.at[b], sib).wait_recv())

    def wait_relay(b, head):
        either(chip == 0, lambda n: remote(piece(b, slice(0, n), head), fwd_s, fwd_r.at[head, b], sib).wait_recv())

    def make_kv(b):
        pos = pos_ref[pl.ds(b, 1), :]
        turns = (pos * high_b[...]).astype(jnp.float32) * (1.0 / TURN) + pos.astype(jnp.float32) * low_b[...]
        turns = turns - jnp.round(turns)
        size = jnp.abs(turns)
        cosine = sin_turns(0.25 - size)
        sine = sin_turns(jnp.minimum(size, 0.5 - size))
        sine = jnp.where(turns < 0, -sine, sine)
        cos_tab = jnp.concatenate([cosine, cosine], axis=0).T
        sin_tab = jnp.concatenate([-sine, sine], axis=0).T
        cos_b[b] = cos_tab
        sin_b[b] = sin_tab
        x_row = xb[b]
        k_row = jnp.dot(x_row, wk[...], preferred_element_type=jnp.float32).astype(jnp.bfloat16)
        v_row = jnp.dot(x_row, wv[...], preferred_element_type=jnp.float32)
        for half, idx in ((0, me), (1, LAST - me)):
            lo = half * BLK
            for g in range(kv_heads):
                cols = slice(g * HEAD_DIM, (g + 1) * HEAD_DIM)
                at = row_at(g)
                kv[b, idx, at:at + BLK, :] = rope_head(k_row[lo:lo + BLK, cols], cos_tab[lo:lo + BLK], sin_tab[lo:lo + BLK])
                kv[b, idx, at + BLK:at + BLK + HEAD_DIM, :] = v_row[lo:lo + BLK, cols].T.astype(jnp.bfloat16)

    def q_tile(b, n):
        cos_tab, sin_tab = cos_b[b], sin_b[b]
        pair = jnp.dot(xb[b], wq[:, n * HEAD_DIM:(n + 2) * HEAD_DIM], preferred_element_type=jnp.float32).astype(jnp.bfloat16)
        for i in range(2):
            ref, h = (q_head, n + i) if n < group else (q_next, n + i - group)
            ref[h] = rope_head(pair[:, i * HEAD_DIM:(i + 1) * HEAD_DIM], cos_tab, sin_tab)

    out_tiles = width // (2 * HEAD_DIM)

    def out_tile(b, n, keep):
        cols = slice(n * 2 * HEAD_DIM, (n + 1) * 2 * HEAD_DIM)
        y_part = jnp.where(keep, jnp.dot(o_full[...], wo[:, cols], preferred_element_type=jnp.float32), 0.0)
        xb[b, :, cols] = (xb[b, :, cols].astype(jnp.float32) + y_part).astype(jnp.bfloat16)

    for copy in (w_copies[4], w_copies[0], x_copy(0)):
        copy.wait()
    for b in range(1, 5):
        x_copy(b).start()
    w_copies[1].wait()
    make_kv(0)
    pl.semaphore_wait(barrier, 2)
    send_row(0)

    def kv_step(i, _):
        at = 2 * i + 1
        x_copy(at).wait()
        x_copy(at + 1).wait()

        @pl.when(i > 0)
        def _():
            send_row(at - 2)
            send_row(at - 1)

        for b in (at + 4, at + 5):
            @pl.when(b < rows)
            def _():
                x_copy(b).start()

        @pl.when(i < 3)
        def _():
            w_piece(wq_hbm, wq, 2, i, 3).start()

        @pl.when(i >= 3)
        def _():
            w_piece(wo_hbm, wo, 3, i - 3, 4).start()

        make_kv(at)
        make_kv(at + 1)
        return _

    lax.fori_loop(0, (rows - 2) // 2, kv_step, None)
    send_row(end - 2)
    send_row(end - 1)
    x_copy(end).wait()
    w_copies[2].wait()
    make_kv(end)
    for n in range(0, q_heads, 2):
        q_tile(0, n)
    send_row(end)
    w_copies[3].wait()

    def spread(step, steps):
        def fill(k, count):
            for n in range(k * steps // count, (k + 1) * steps // count):
                step(n)
        return fill

    def row_step(b, _):
        b_old = jnp.maximum(b - 1, 0)
        relay(b, 0)

        @pl.when(b > 0)
        def _():
            wait_relay(b_old, 1)

        for dev in range(CP_SIZE):
            @pl.when((me == dev) & (b > 0))
            def _():
                o_full[:, :head_cols] = o_head[...]
                attend(kv.at[b_old], row_at(1), q_tail, o_full, head_cols, sb, dev, spread(lambda n: q_tile(b, 2 * n), q_heads // 2))

        wait_sib(b)
        wait_relay(b, 0)
        relay(b, 1)
        for dev in range(CP_SIZE):
            @pl.when((me == dev) & (b < end))
            def _():
                q_tail[...] = q_next[...]
                attend(kv.at[b], row_at(0), q_head, o_head, 0, sb, dev, spread(lambda n: out_tile(b_old, n, b > 0), out_tiles))

        return _

    lax.fori_loop(0, rows, row_step, None)
    kv_end[:, :row_at(1), :] = kv[end, :, :row_at(1), :]
    wait_relay(end, 1)
    kv_end[:, row_at(1):, :] = kv[end, :, row_at(1):, :]

    either(chip == 1, lambda n: remote(kv.at[:, 0:n], ici_s, ici_r.at[0, 0], par).wait_send())
    either(chip == 0, lambda n: remote(kv.at[:, 0:n], fwd_s, fwd_r.at[0, 0], sib).wait_send())
    either(core == 1, lambda n: remote(kv.at[:, 0:n], sib_s, sib_r.at[0], sib).wait_send())


def end_kernel(xb, wo, kv_end, q_head, q_tail, o_full, y_hbm, sb, o_head, o_tail, acc, y_rows, sem):
    rows, toks, width = xb.shape
    end = rows - 1
    me = lax.axis_index("cp")
    copies = [pltpu.make_async_copy(xb.at[b], y_hbm.at[b], sem.at[b]) for b in range(end - 1)]
    for copy in copies:
        copy.start()
    old = o_head.shape[1]
    tile = 2 * HEAD_DIM
    out_tiles = width // tile

    def spread(step):
        def fill(k, count):
            for n in range(k * out_tiles // count, (k + 1) * out_tiles // count):
                step(slice(n * tile, (n + 1) * tile))
        return fill

    def out_before(cols):
        y_part = jnp.dot(o_full[...], wo[:, cols], preferred_element_type=jnp.float32)
        y_rows[0, :, cols] = (xb[end - 1, :, cols].astype(jnp.float32) + y_part).astype(jnp.bfloat16)

    def out_head(cols):
        acc[:, cols] = xb[end, :, cols].astype(jnp.float32) + jnp.dot(o_head[...], wo[:old, cols], preferred_element_type=jnp.float32)

    for dev in range(CP_SIZE):
        @pl.when(me == dev)
        def _():
            attend(kv_end, 0, q_head, o_head, 0, sb, dev, spread(out_before))
            attend(kv_end, BLK + HEAD_DIM, q_tail, o_tail, 0, sb, dev, spread(out_head))

    copies.append(pltpu.make_async_copy(y_rows.at[0], y_hbm.at[end - 1], sem.at[end - 1]))
    copies[-1].start()
    for n in range(out_tiles):
        cols = slice(n * tile, (n + 1) * tile)
        y_rows[1, :, cols] = (acc[:, cols] + jnp.dot(o_tail[...], wo[old:, cols], preferred_element_type=jnp.float32)).astype(jnp.bfloat16)
        if n % 2:
            span = slice((n - 1) * tile, (n + 1) * tile)
            copies.append(pltpu.make_async_copy(y_rows.at[1, :, span], y_hbm.at[end, :, span], sem.at[end + n // 2]))
            copies[-1].start()
    for copy in copies:
        copy.wait()


def solution(mesh):
    row_spec = P('data', 'cp', None)
    pos_spec = P('data', 'cp')
    rep_spec = P(None, None)

    def local_block(x_loc, pos_loc, w_query, w_key, w_value, w_out):
        rows, toks, width = x_loc.shape
        q_cols, kv_cols = w_query.shape[1], w_key.shape[1]
        group = q_cols // kv_cols
        any_spec = pl.BlockSpec(memory_space=pl.ANY)
        vmem_spec = pl.BlockSpec(memory_space=pltpu.VMEM)
        bf16, f32 = jnp.bfloat16, jnp.float32
        one_sem = pltpu.SemaphoreType.DMA
        head_sem = pltpu.SemaphoreType.DMA((kv_cols // HEAD_DIM, rows))
        row_sem = pltpu.SemaphoreType.DMA((rows,))
        kept = pl.pallas_call(
            main_kernel,
            out_shape=[
                pltpu.VMEM(x_loc.shape, bf16),
                pltpu.VMEM((q_cols, width), bf16),
                pltpu.VMEM((2 * CP_SIZE, 2 * kv_cols, BLK), bf16),
                pltpu.VMEM((group, toks, HEAD_DIM), bf16),
                pltpu.VMEM((group, toks, HEAD_DIM), bf16),
                pltpu.VMEM((toks, q_cols), bf16),
            ],
            in_specs=[any_spec] * 6,
            out_specs=[vmem_spec] * 6,
            scratch_shapes=[
                pltpu.VMEM((width, q_cols), bf16),
                pltpu.VMEM((width, kv_cols), bf16),
                pltpu.VMEM((width, kv_cols), bf16),
                pltpu.VMEM((rows, 2 * CP_SIZE, 2 * kv_cols, BLK), bf16),
                pltpu.VMEM((group, toks, HEAD_DIM), bf16),
                pltpu.VMEM((toks, group * HEAD_DIM), bf16),
                pltpu.VMEM((4 * CP_SIZE * toks, 2 * BLK), f32),
                pltpu.VMEM((rows, toks), jnp.int32),
                pltpu.VMEM((HALF_DIM, toks), jnp.int32),
                pltpu.VMEM((HALF_DIM, toks), f32),
                pltpu.VMEM((rows, toks, HEAD_DIM), f32),
                pltpu.VMEM((rows, toks, HEAD_DIM), f32),
                row_sem, pltpu.SemaphoreType.DMA((5,)),
                one_sem, head_sem, one_sem, row_sem, one_sem, head_sem,
            ],
            compiler_params=pltpu.CompilerParams(collective_id=0, has_side_effects=True, vmem_limit_bytes=43 * 1024 * 1024),
        )(x_loc, pos_loc, w_query, w_key, w_value, w_out)
        return pl.pallas_call(
            end_kernel,
            out_shape=jax.ShapeDtypeStruct(x_loc.shape, bf16),
            in_specs=[vmem_spec] * 6,
            out_specs=any_spec,
            scratch_shapes=[
                pltpu.VMEM((4 * CP_SIZE * toks, 2 * BLK), f32),
                pltpu.VMEM((toks, group * HEAD_DIM), bf16),
                pltpu.VMEM((toks, group * HEAD_DIM), bf16),
                pltpu.VMEM((toks, width), f32),
                pltpu.VMEM((2, toks, width), bf16),
                pltpu.SemaphoreType.DMA((rows + 2,)),
            ],
            compiler_params=pltpu.CompilerParams(vmem_limit_bytes=16 * 1024 * 1024),
        )(*kept)

    return jax.shard_map(local_block, mesh=mesh, in_specs=(row_spec, pos_spec, rep_spec, rep_spec, rep_spec, rep_spec), out_specs=row_spec, check_vma=False)
```

```python
import math

import jax
import jax.numpy as jnp
import numpy as np
from jax import lax
from jax.experimental import pallas as pl
from jax.experimental.pallas import tpu as pltpu
from jax.sharding import PartitionSpec as P

HEAD_DIM = 128
HALF_DIM = HEAD_DIM // 2
ROPE_BASE = 500000
MASK_FILL = -1e30
EXP_SCALE = math.log2(math.e) * HEAD_DIM ** -0.5
CP_SIZE = 4
LAST = 2 * CP_SIZE - 1
BLK = 128
LEAD = 3
MESH = pl.DeviceIdType.MESH
TURN = 2.0 ** 32
SIN_COEF = [(-1) ** k * (2 * math.pi) ** (2 * k + 1) / math.factorial(2 * k + 1) for k in range(7)]


def turn_tables(toks):
    turns = ROPE_BASE ** (-np.arange(0, HEAD_DIM, 2, dtype=np.float64) / HEAD_DIM) / (2 * math.pi)
    high = np.floor(turns * TURN)
    low = turns - high / TURN
    sub = 8
    lane_row = lax.broadcasted_iota(jnp.int32, (sub, toks), 0)
    parts = ([], [])
    for a in range(0, HALF_DIM, sub):
        for part, values, kind, num in zip(parts, (high, low), (jnp.int32, jnp.float32), (int, float)):
            tile = jnp.full((sub, toks), num(values[a]), kind)
            for c in range(1, sub):
                tile = jnp.where(lane_row == c, jnp.full((sub, toks), num(values[a + c]), kind), tile)
            part.append(tile)
    return [jnp.concatenate(part, axis=0) for part in parts]


def sin_turns(part):
    square = part * part
    total = jnp.full_like(part, SIN_COEF[-1])
    for coef in SIN_COEF[-2::-1]:
        total = total * square + coef
    return total * part


def nt_dot(lhs, rhs):
    return lax.dot_general(lhs, rhs, (((1,), (1,)), ((), ())), preferred_element_type=jnp.float32)


def rope_head(head, cos_tab, sin_tab):
    wide = head.astype(jnp.float32)
    return (wide * cos_tab + pltpu.roll(wide, HALF_DIM, 1) * sin_tab).astype(jnp.bfloat16)


def attend(kv_row, row_of, q_row, o_row, o_col, sb, dev, fill):
    wide = (BLK, 2 * BLK)
    tri = lax.broadcasted_iota(jnp.int32, wide, 0) <= lax.rem(lax.broadcasted_iota(jnp.int32, wide, 1), BLK)
    units = [(half, h) for half in (1, 0) for h in range(0, q_row.shape[0], 2)]

    def spans(half):
        n_blk = LAST - dev + 1 if half else dev + 1
        return n_blk, n_blk * BLK, slice(half * BLK, (half + 1) * BLK)

    starts, at = [], 0
    for half, _ in units:
        need = spans(half)[1]
        at = 0 if at + need > sb.shape[0] else at
        starts.append(at)
        at += need

    def score(k):
        half, h = units[k]
        n_blk, n_key, toks_at = spans(half)
        base = starts[k]
        keys = kv_row[0:n_blk, row_of:row_of + BLK, :].reshape(n_key, HEAD_DIM)
        scores = nt_dot(keys, q_row[h:h + 2, toks_at, :].reshape(2 * BLK, HEAD_DIM))
        diag = jnp.where(tri, scores[n_key - BLK:], MASK_FILL)
        sb[base + n_key - BLK:base + n_key, :] = diag
        top = jnp.max(diag, axis=0, keepdims=True)
        if n_blk > 1:
            sb[base:base + n_key - BLK, :] = scores[:n_key - BLK]
            top = jnp.maximum(top, jnp.max(scores[:n_key - BLK], axis=0, keepdims=True))
        return top

    def weigh(k, top):
        half, h = units[k]
        n_blk, n_key, toks_at = spans(half)
        exp_w = jnp.exp2((sb[starts[k]:starts[k] + n_key, :] - top) * EXP_SCALE)
        inv = 1.0 / jnp.sum(exp_w, axis=0, keepdims=True)
        lo = row_of + BLK
        vals = jnp.concatenate([kv_row[i, lo:lo + HEAD_DIM, :] for i in range(n_blk)], axis=1)
        out = (jnp.dot(vals, exp_w.astype(jnp.bfloat16), preferred_element_type=jnp.float32) * inv).T.astype(jnp.bfloat16)
        for i in range(2):
            o_row[toks_at, o_col + (h + i) * HEAD_DIM:o_col + (h + i + 1) * HEAD_DIM] = out[i * BLK:(i + 1) * BLK]

    count = len(units)
    tops = [score(k) for k in range(LEAD)]
    for k in range(count):
        if k + LEAD < count:
            tops.append(score(k + LEAD))
        weigh(k, tops[k])
        fill(k, count)


def main_kernel(x_hbm, pos_hbm, wq_hbm, wk_hbm, wv_hbm, wo_hbm, xb, wo, kv_end, q_head, q_next, o_full,
                wq, wk, wv, kv, q_tail, o_head, sb, pos_ref, high_b, low_b, cos_b, sin_b,
                xsem, wsem, ici_s, ici_r, sib_s, sib_r, fwd_s, fwd_r):
    rows, toks, width = xb.shape
    kv_cols = wk.shape[1]
    kv_heads = kv_cols // HEAD_DIM
    q_heads = wq.shape[1] // HEAD_DIM
    group = q_heads // kv_heads
    head_cols = group * HEAD_DIM
    end = rows - 1
    me = lax.axis_index("cp")
    chip = me // 2
    core = lax.rem(me, 2)
    sib = chip * 2 + (1 - core)
    par = (1 - chip) * 2 + core
    dia = (1 - chip) * 2 + (1 - core)

    w_copies = [pltpu.make_async_copy(src, dst, wsem.at[i]) for i, (src, dst) in enumerate(((wk_hbm, wk), (wv_hbm, wv), (wq_hbm, wq), (wo_hbm, wo), (pos_hbm, pos_ref)))]

    def x_copy(b):
        return pltpu.make_async_copy(x_hbm.at[b], xb.at[b], xsem.at[b])

    def w_piece(src, dst, i, at, count):
        depth = src.shape[0] // count
        part = pl.ds(pl.multiple_of(at * depth, depth), depth)
        return pltpu.make_async_copy(src.at[part], dst.at[part], wsem.at[i])

    w_copies[0].start()
    x_copy(0).start()
    w_copies[1].start()
    w_copies[4].start()
    barrier = pltpu.get_barrier_semaphore()
    for other in (sib, par):
        pl.semaphore_signal(barrier, inc=1, device_id={"cp": other}, device_id_type=MESH)
    high_b[...], low_b[...] = turn_tables(toks)

    def row_at(g):
        return g * (BLK + HEAD_DIM)

    def piece(b, idx, head):
        return kv.at[b, idx] if head is None else kv.at[b, idx, row_at(head):row_at(head + 1)]

    def remote(ref, send, recv, dev):
        return pltpu.make_async_remote_copy(src_ref=ref, dst_ref=ref, send_sem=send, recv_sem=recv, device_id={"cp": dev}, device_id_type=MESH)

    def either(twin, act):
        @pl.when(twin)
        def _():
            act(2)

        @pl.when(jnp.logical_not(twin))
        def _():
            act(1)

    def send_row(b):
        for head in range(kv_heads):
            remote(piece(b, me, head), ici_s, ici_r.at[head, b], par).start()

            @pl.when(chip == 1)
            def _():
                remote(piece(b, LAST - me, head), ici_s, ici_r.at[head, b], par).start()

        remote(piece(b, me, None), sib_s, sib_r.at[b], sib).start()

        @pl.when(core == 1)
        def _():
            remote(piece(b, LAST - me, None), sib_s, sib_r.at[b], sib).start()

    def relay(b, head):
        either(chip == 0, lambda n: remote(piece(b, slice(0, n), head), ici_s, ici_r.at[head, b], par).wait_recv())
        remote(piece(b, par, head), fwd_s, fwd_r.at[head, b], sib).start()

        @pl.when(chip == 0)
        def _():
            remote(piece(b, LAST - par, head), fwd_s, fwd_r.at[head, b], sib).start()

    def wait_sib(b):
        either(core == 0, lambda n: remote(piece(b, slice(0, n), None), sib_s, sib_r.at[b], sib).wait_recv())

    def wait_relay(b, head):
        either(chip == 0, lambda n: remote(piece(b, slice(0, n), head), fwd_s, fwd_r.at[head, b], sib).wait_recv())

    def make_kv(b):
        pos = pos_ref[pl.ds(b, 1), :]
        turns = (pos * high_b[...]).astype(jnp.float32) * (1.0 / TURN) + pos.astype(jnp.float32) * low_b[...]
        turns = turns - jnp.round(turns)
        size = jnp.abs(turns)
        cosine = sin_turns(0.25 - size)
        sine = sin_turns(jnp.minimum(size, 0.5 - size))
        sine = jnp.where(turns < 0, -sine, sine)
        cos_tab = jnp.concatenate([cosine, cosine], axis=0).T
        sin_tab = jnp.concatenate([-sine, sine], axis=0).T
        cos_b[b] = cos_tab
        sin_b[b] = sin_tab
        x_row = xb[b]
        k_row = jnp.dot(x_row, wk[...], preferred_element_type=jnp.float32).astype(jnp.bfloat16)
        v_row = jnp.dot(x_row, wv[...], preferred_element_type=jnp.float32)
        for half, idx in ((0, me), (1, LAST - me)):
            lo = half * BLK
            for g in range(kv_heads):
                cols = slice(g * HEAD_DIM, (g + 1) * HEAD_DIM)
                at = row_at(g)
                kv[b, idx, at:at + BLK, :] = rope_head(k_row[lo:lo + BLK, cols], cos_tab[lo:lo + BLK], sin_tab[lo:lo + BLK])
                kv[b, idx, at + BLK:at + BLK + HEAD_DIM, :] = v_row[lo:lo + BLK, cols].T.astype(jnp.bfloat16)

    def q_tile(b, n):
        cos_tab, sin_tab = cos_b[b], sin_b[b]
        pair = jnp.dot(xb[b], wq[:, n * HEAD_DIM:(n + 2) * HEAD_DIM], preferred_element_type=jnp.float32).astype(jnp.bfloat16)
        for i in range(2):
            ref, h = (q_head, n + i) if n < group else (q_next, n + i - group)
            ref[h] = rope_head(pair[:, i * HEAD_DIM:(i + 1) * HEAD_DIM], cos_tab, sin_tab)

    out_tiles = width // (2 * HEAD_DIM)

    def out_tile(b, n, keep):
        cols = slice(n * 2 * HEAD_DIM, (n + 1) * 2 * HEAD_DIM)
        y_part = jnp.where(keep, jnp.dot(o_full[...], wo[:, cols], preferred_element_type=jnp.float32), 0.0)
        xb[b, :, cols] = (xb[b, :, cols].astype(jnp.float32) + y_part).astype(jnp.bfloat16)

    for copy in (w_copies[4], w_copies[0], x_copy(0)):
        copy.wait()
    w_copies[1].wait()
    for b in range(1, 5):
        x_copy(b).start()
    pl.semaphore_wait(barrier, 2)
    make_kv(0)
    send_row(0)

    def kv_step(i, _):
        at = 2 * i + 1
        x_copy(at).wait()
        x_copy(at + 1).wait()

        @pl.when(i > 0)
        def _():
            send_row(at - 2)
            send_row(at - 1)

        for b in (at + 4, at + 5):
            @pl.when(b < rows)
            def _():
                x_copy(b).start()

        @pl.when(i < 3)
        def _():
            w_piece(wq_hbm, wq, 2, i, 3).start()

        @pl.when(i >= 3)
        def _():
            w_piece(wo_hbm, wo, 3, i - 3, 4).start()

        make_kv(at)
        make_kv(at + 1)
        return _

    lax.fori_loop(0, (rows - 2) // 2, kv_step, None)
    send_row(end - 2)
    send_row(end - 1)
    x_copy(end).wait()
    w_copies[2].wait()
    make_kv(end)
    for n in range(0, q_heads, 2):
        q_tile(0, n)
    send_row(end)
    w_copies[3].wait()

    def spread(step, steps):
        def fill(k, count):
            for n in range(k * steps // count, (k + 1) * steps // count):
                step(n)
        return fill

    def row_step(b, _):
        b_old = jnp.maximum(b - 1, 0)
        relay(b, 0)

        @pl.when(b > 0)
        def _():
            wait_relay(b_old, 1)

        for dev in range(CP_SIZE):
            @pl.when((me == dev) & (b > 0))
            def _():
                o_full[:, :head_cols] = o_head[...]
                attend(kv.at[b_old], row_at(1), q_tail, o_full, head_cols, sb, dev, spread(lambda n: q_tile(b, 2 * n), q_heads // 2))

        wait_sib(b)
        wait_relay(b, 0)
        relay(b, 1)
        for dev in range(CP_SIZE):
            @pl.when((me == dev) & (b < end))
            def _():
                q_tail[...] = q_next[...]
                attend(kv.at[b], row_at(0), q_head, o_head, 0, sb, dev, spread(lambda n: out_tile(b_old, n, b > 0), out_tiles))

        return _

    lax.fori_loop(0, rows, row_step, None)
    kv_end[:, :row_at(1), :] = kv[end, :, :row_at(1), :]
    wait_relay(end, 1)
    kv_end[:, row_at(1):, :] = kv[end, :, row_at(1):, :]

    either(chip == 1, lambda n: remote(kv.at[:, 0:n], ici_s, ici_r.at[0, 0], par).wait_send())
    either(chip == 0, lambda n: remote(kv.at[:, 0:n], fwd_s, fwd_r.at[0, 0], sib).wait_send())
    either(core == 1, lambda n: remote(kv.at[:, 0:n], sib_s, sib_r.at[0], sib).wait_send())


def end_kernel(xb, wo, kv_end, q_head, q_tail, o_full, y_hbm, sb, o_head, o_tail, acc, y_rows, sem):
    rows, toks, width = xb.shape
    end = rows - 1
    me = lax.axis_index("cp")
    copies = [pltpu.make_async_copy(xb.at[b], y_hbm.at[b], sem.at[b]) for b in range(end - 1)]
    for copy in copies:
        copy.start()
    old = o_head.shape[1]
    tile = 2 * HEAD_DIM
    out_tiles = width // tile

    def spread(step):
        def fill(k, count):
            for n in range(k * out_tiles // count, (k + 1) * out_tiles // count):
                step(slice(n * tile, (n + 1) * tile))
        return fill

    def out_before(cols):
        y_part = jnp.dot(o_full[...], wo[:, cols], preferred_element_type=jnp.float32)
        y_rows[0, :, cols] = (xb[end - 1, :, cols].astype(jnp.float32) + y_part).astype(jnp.bfloat16)

    def out_head(cols):
        acc[:, cols] = xb[end, :, cols].astype(jnp.float32) + jnp.dot(o_head[...], wo[:old, cols], preferred_element_type=jnp.float32)

    for dev in range(CP_SIZE):
        @pl.when(me == dev)
        def _():
            attend(kv_end, 0, q_head, o_head, 0, sb, dev, spread(out_before))
            attend(kv_end, BLK + HEAD_DIM, q_tail, o_tail, 0, sb, dev, spread(out_head))

    copies.append(pltpu.make_async_copy(y_rows.at[0], y_hbm.at[end - 1], sem.at[end - 1]))
    copies[-1].start()
    for n in range(out_tiles):
        cols = slice(n * tile, (n + 1) * tile)
        y_rows[1, :, cols] = (acc[:, cols] + jnp.dot(o_tail[...], wo[old:, cols], preferred_element_type=jnp.float32)).astype(jnp.bfloat16)
        if n % 2:
            span = slice((n - 1) * tile, (n + 1) * tile)
            copies.append(pltpu.make_async_copy(y_rows.at[1, :, span], y_hbm.at[end, :, span], sem.at[end + n // 2]))
            copies[-1].start()
    for copy in copies:
        copy.wait()


def solution(mesh):
    row_spec = P('data', 'cp', None)
    pos_spec = P('data', 'cp')
    rep_spec = P(None, None)

    def local_block(x_loc, pos_loc, w_query, w_key, w_value, w_out):
        rows, toks, width = x_loc.shape
        q_cols, kv_cols = w_query.shape[1], w_key.shape[1]
        group = q_cols // kv_cols
        any_spec = pl.BlockSpec(memory_space=pl.ANY)
        vmem_spec = pl.BlockSpec(memory_space=pltpu.VMEM)
        bf16, f32 = jnp.bfloat16, jnp.float32
        one_sem = pltpu.SemaphoreType.DMA
        head_sem = pltpu.SemaphoreType.DMA((kv_cols // HEAD_DIM, rows))
        row_sem = pltpu.SemaphoreType.DMA((rows,))
        kept = pl.pallas_call(
            main_kernel,
            out_shape=[
                pltpu.VMEM(x_loc.shape, bf16),
                pltpu.VMEM((q_cols, width), bf16),
                pltpu.VMEM((2 * CP_SIZE, 2 * kv_cols, BLK), bf16),
                pltpu.VMEM((group, toks, HEAD_DIM), bf16),
                pltpu.VMEM((group, toks, HEAD_DIM), bf16),
                pltpu.VMEM((toks, q_cols), bf16),
            ],
            in_specs=[any_spec] * 6,
            out_specs=[vmem_spec] * 6,
            scratch_shapes=[
                pltpu.VMEM((width, q_cols), bf16),
                pltpu.VMEM((width, kv_cols), bf16),
                pltpu.VMEM((width, kv_cols), bf16),
                pltpu.VMEM((rows, 2 * CP_SIZE, 2 * kv_cols, BLK), bf16),
                pltpu.VMEM((group, toks, HEAD_DIM), bf16),
                pltpu.VMEM((toks, group * HEAD_DIM), bf16),
                pltpu.VMEM((4 * CP_SIZE * toks, 2 * BLK), f32),
                pltpu.VMEM((rows, toks), jnp.int32),
                pltpu.VMEM((HALF_DIM, toks), jnp.int32),
                pltpu.VMEM((HALF_DIM, toks), f32),
                pltpu.VMEM((rows, toks, HEAD_DIM), f32),
                pltpu.VMEM((rows, toks, HEAD_DIM), f32),
                row_sem, pltpu.SemaphoreType.DMA((5,)),
                one_sem, head_sem, one_sem, row_sem, one_sem, head_sem,
            ],
            compiler_params=pltpu.CompilerParams(collective_id=0, has_side_effects=True, vmem_limit_bytes=43 * 1024 * 1024),
        )(x_loc, pos_loc, w_query, w_key, w_value, w_out)
        return pl.pallas_call(
            end_kernel,
            out_shape=jax.ShapeDtypeStruct(x_loc.shape, bf16),
            in_specs=[vmem_spec] * 6,
            out_specs=any_spec,
            scratch_shapes=[
                pltpu.VMEM((4 * CP_SIZE * toks, 2 * BLK), f32),
                pltpu.VMEM((toks, group * HEAD_DIM), bf16),
                pltpu.VMEM((toks, group * HEAD_DIM), bf16),
                pltpu.VMEM((toks, width), f32),
                pltpu.VMEM((2, toks, width), bf16),
                pltpu.SemaphoreType.DMA((rows + 2,)),
            ],
            compiler_params=pltpu.CompilerParams(vmem_limit_bytes=16 * 1024 * 1024),
        )(*kept)

    return jax.shard_map(local_block, mesh=mesh, in_specs=(row_spec, pos_spec, rep_spec, rep_spec, rep_spec, rep_spec), out_specs=row_spec, check_vma=False)
```
